256 devices in a mesh: section: 4 (over x), tok: 32 (over z, y), head: 2 (over core).
Axes of the slice: x: 4, y: 4, z: 8, core: 2. Of those that a mesh axis runs over, the one named last changes fastest.
Arguments:
- group_in: bfloat16 [4, 4096, 2048], P('section', 'tok'), may hold values from -6 to 6
- w_qkv: bfloat16 [4, 3, 2048, 2048], P('section', None, 'tok', 'head'), may hold values from -0.125 to 0.125
- w_out: bfloat16 [4, 2048, 2048], P('section', 'head', 'tok'), may hold values from -0.125 to 0.125
- step_sizes: float32 [4, 4096, 4], P('section', 'tok', 'head'), may hold values from 0.05 to 1
- fast_weights: bfloat16 [4, 4, 3, 512, 512], P('section', 'head'), may hold values from -0.25 to 0.25
- momentum: bfloat16 [4, 4, 3, 512, 512], P('section', 'head'), may hold values from -48 to 48
- momentum_decay: float32 [4, 4], P('section', 'head'), may hold values from 0.5 to 0.95
- fast_rate: float32 [4, 4], P('section', 'head'), may hold values from 0.3 to 1
Outputs:
- handed: bfloat16 [4, 4096, 2048], P('section', 'tok', 'head')
- fast_next: bfloat16 [4, 4, 3, 512, 512], P('section', 'head')
The draws below stay inside these ranges and needn't reach their ends.
All inputs are finite; a program needn't handle non-finite values.
Results may differ from the reference program's by a relative error of at most 0.015.
Values may be sent and summed in bfloat16 or wider, within the bound.
No kernel may reach another device: no remote copies, remote signals or barrier semaphores. Data moves between devices by JAX's collectives and lax.ppermute only.
A program may use at most 128 MiB of HBM per device.

```python
import math
import jax
import jax.numpy as jnp
from jax import lax

D = 2048
HEADS = 4
FIN = 512
FH = 512
NS_ITERS = 2
SECTIONS = 4
GROUP = 4096


def level_of(rng, dims, pieces, smallest, largest):
    loudness = 1.0
    for position, parts in pieces:
        draws = jax.random.uniform(jax.random.fold_in(jax.random.fold_in(rng, 6), position), (parts,), jnp.float32, smallest / len(pieces), largest / len(pieces))
        loudness = loudness * jnp.repeat(jnp.exp(draws), dims[position] // parts).reshape((-1,) + (1,) * (len(dims) - 1 - position))
    return loudness


def normal_values(own_key, dims, width, bound, pieces=(), held_as=jnp.bfloat16):
    result = jax.random.normal(own_key, dims, jnp.float32) * width
    if len(pieces) > 0:
        result = level_of(own_key, dims, pieces, -0.22, 0.18) * result
    return jnp.clip(result, min=-bound, max=bound).astype(held_as)


def setup_inputs(seed: int = 0) -> dict:
    streams_of = jax.random.split(jax.random.key(seed), 9)
    return {
        "group_in": normal_values(streams_of[0], (SECTIONS, GROUP, D), 1.0, 6.0, ((0, 4), (1, 32))),
        "w_qkv": normal_values(streams_of[1], (SECTIONS, 3, D, D), D ** -0.5, 0.125, ((0, 4), (2, 32), (3, 2))),
        "w_out": normal_values(streams_of[2], (SECTIONS, D, D), D ** -0.5, 0.125, ((0, 4), (1, 2), (2, 32))),
        "step_sizes": jnp.clip(jnp.exp(math.log(1.0) - 2.9957323 * jax.random.uniform(streams_of[3], (SECTIONS, GROUP, HEADS), jnp.float32) ** level_of(streams_of[3], (SECTIONS, GROUP, HEADS), ((0, 4), (1, 32), (2, 2)), -0.2, 0.2)), 0.05, 1.0),
        "fast_weights": normal_values(streams_of[4], (SECTIONS, HEADS, 3, FIN, FH), FIN ** -0.5, 0.25, ((0, 4), (1, 2))),
        "momentum": normal_values(streams_of[5], (SECTIONS, HEADS, 3, FIN, FH), (GROUP ** 0.5 * 0.125), 48.0, ((0, 4), (1, 2))),
        "momentum_decay": jnp.clip(0.5 + 0.45 * jax.random.uniform(streams_of[6], (SECTIONS, HEADS), jnp.float32) ** level_of(streams_of[6], (SECTIONS, HEADS), ((0, 4), (1, 2)), -0.2, 0.2), 0.5, 0.95),
        "fast_rate": jnp.clip(jnp.exp(math.log(1.0) - 1.2039728 * jax.random.uniform(streams_of[7], (SECTIONS, HEADS), jnp.float32) ** level_of(streams_of[7], (SECTIONS, HEADS), ((0, 4), (1, 2)), -0.2, 0.2)), 0.3, 1.0),
    }


coef_linear = 3.4445
coef_cubic = -4.775
coef_quintic = 2.0315

def rms_rows(values_in, epsilon):
    return values_in * lax.rsqrt(lax.optimization_barrier(jnp.mean(values_in * values_in, axis=-1, keepdims=True)) + epsilon)

def fast_grads(key_rows, value_rows, step_rates, weights):
    key_wide = key_rows.astype(jnp.float32)
    weight_wide = weights.astype(jnp.float32)
    gate_pre = jnp.einsum('thi,hij->thj', key_wide, weight_wide[:, 0])
    up_pre = jnp.einsum('thi,hij->thj', key_wide, weight_wide[:, 1])
    squash = jax.nn.sigmoid(gate_pre)
    hidden = (gate_pre * squash * up_pre).astype(jnp.bfloat16)
    errors = (-(step_rates[:, :, None] * value_rows.astype(jnp.float32))).astype(jnp.bfloat16)
    errors_wide = errors.astype(jnp.float32)
    back_hidden = jnp.einsum('thi,hij->thj', errors_wide, weight_wide[:, 2])
    grad_gate = (back_hidden * up_pre * squash * (1.0 + gate_pre * (1.0 - squash))).astype(jnp.bfloat16)
    grad_up = (back_hidden * gate_pre * squash).astype(jnp.bfloat16)
    grad_first = jnp.einsum('thi,thj->hij', key_wide, grad_gate.astype(jnp.float32))
    grad_third = jnp.einsum('thi,thj->hij', key_wide, grad_up.astype(jnp.float32))
    grad_second = jnp.einsum('thi,thj->hij', errors_wide, hidden.astype(jnp.float32))
    return jnp.stack([grad_first, grad_third, grad_second], axis=1)

def newton_step(iterate):
    iterate_wide = iterate.astype(jnp.float32)
    gram_matrix = jnp.einsum('mij,mik->mjk', iterate_wide, iterate_wide).astype(jnp.bfloat16)
    gram_wide = gram_matrix.astype(jnp.float32)
    cubic_term = jnp.einsum('mij,mjk->mik', iterate_wide, gram_wide)
    rounded = lax.optimization_barrier(cubic_term.astype(jnp.bfloat16))
    quintic_term = jnp.einsum('mij,mjk->mik', rounded.astype(jnp.float32), gram_wide)
    return (coef_linear * iterate_wide + coef_cubic * cubic_term + coef_quintic * quintic_term).astype(jnp.bfloat16)

def apply_fast(queries, updated):
    query_wide = queries.astype(jnp.float32)
    weight_wide = updated.astype(jnp.float32)
    gate_pre = jnp.einsum('thi,hij->thj', query_wide, weight_wide[:, 0])
    up_pre = jnp.einsum('thi,hij->thj', query_wide, weight_wide[:, 1])
    hidden = (jax.nn.silu(gate_pre) * up_pre).astype(jnp.bfloat16)
    output = jnp.einsum('thj,hij->thi', hidden.astype(jnp.float32), weight_wide[:, 2])
    return rms_rows(output, 1e-05).astype(jnp.bfloat16).reshape(GROUP, HEADS * FIN)

def reference(group_in, w_qkv, w_out, step_sizes, fast_weights, momentum, momentum_decay, fast_rate):
    outs_list = []
    weights_list = []
    for level_index in range(SECTIONS):
        tokens = group_in[level_index]
        projected = [jnp.dot(tokens, w_qkv[level_index, component], preferred_element_type=jnp.float32) for component in range(3)]
        queries = rms_rows(projected[0].reshape(GROUP, HEADS, FIN), 1e-06).astype(jnp.bfloat16)
        key_rows = rms_rows(projected[1].reshape(GROUP, HEADS, FIN), 1e-06).astype(jnp.bfloat16)
        value_rows = projected[2].reshape(GROUP, HEADS, FIN).astype(jnp.bfloat16)
        gradients = fast_grads(key_rows, value_rows, step_sizes[level_index], fast_weights[level_index])
        moment = momentum_decay[level_index][:, None, None, None] * momentum[level_index].astype(jnp.float32) + gradients
        norm_values = jnp.sqrt(lax.optimization_barrier(jnp.sum(moment * moment, axis=(2, 3), keepdims=True)))
        iterate = (moment / (norm_values + 1e-06)).astype(jnp.bfloat16).reshape(HEADS * 3, FIN, FH)
        for number in range(NS_ITERS):
            iterate = newton_step(iterate)
        iterate = iterate.reshape(HEADS, 3, FIN, FH)
        updated = (fast_weights[level_index].astype(jnp.float32) - fast_rate[level_index][:, None, None, None] * iterate.astype(jnp.float32)).astype(jnp.bfloat16)
        mixed_heads = apply_fast(queries, updated)
        layer_out = (tokens.astype(jnp.float32) + jnp.dot(mixed_heads, w_out[level_index], preferred_element_type=jnp.float32)).astype(jnp.bfloat16)
        outs_list.append(layer_out)
        weights_list.append(updated)
    stacked = jnp.stack(outs_list)
    handed = jnp.roll(stacked, 1, axis=0)
    return (handed, jnp.stack(weights_list))
```

```python
import jax
import jax.numpy as jnp
from jax import lax
from jax.experimental import pallas as pl
from jax.experimental.pallas import tpu as pltpu
from jax.sharding import Mesh
from jax.sharding import PartitionSpec as P

NS_ITERS = 2
TOK = ("z", "y")

coef_linear = 3.4445
coef_cubic = -4.775
coef_quintic = 2.0315

bf16 = jnp.bfloat16
f32 = jnp.float32


def moved(value, axis, steps):
    count = lax.axis_size(axis)
    return lax.ppermute(value, axis, [(i, (i + steps) % count) for i in range(count)])


def swapped(value):
    return lax.ppermute(value, "head", [(0, 1), (1, 0)])


def dot(a, b, ca, cb):
    return lax.dot_general(a, b, (((ca,), (cb,)), ((), ())), preferred_element_type=f32)


def kernel_call(body, name, outs, args, flops=0, scratch=(), limit=24):
    size = sum(a.size * a.dtype.itemsize for a in args[1:])
    return pl.pallas_call(
        body,
        name=name,
        out_shape=outs,
        in_specs=[pl.BlockSpec(memory_space=pltpu.SMEM)]
        + [pl.BlockSpec(memory_space=pltpu.VMEM)] * (len(args) - 1),
        out_specs=jax.tree.map(lambda _: pl.BlockSpec(memory_space=pltpu.VMEM), outs),
        scratch_shapes=list(scratch),
        compiler_params=pltpu.CompilerParams(vmem_limit_bytes=limit << 20),
        cost_estimate=pl.CostEstimate(flops=flops, bytes_accessed=size, transcendentals=0),
    )(*args)


def shape(*dims, dtype=bf16):
    return jax.ShapeDtypeStruct(dims, dtype)


def pack_body(place, w_ref, o_ref, extra_ref, *outs):
    y = place[0]
    for k, out in enumerate(outs):
        j = lax.rem(y + k, 4)
        columns = pl.ds(pl.multiple_of(j * 256, 256), 256)
        for row, component in enumerate((1, 2, 0)):
            out[row * 64 : row * 64 + 64, :] = w_ref[component, :, columns]
        out[192:256, :] = o_ref[:, columns]
        out[256:264, :] = extra_ref[lax.div(j, 2)]


def sort_body(place, a, b, c, d, kv, qo, steps):
    slot = 2 * lax.rem(place[0], 2) + place[2]
    for k, piece in enumerate((a, b, c, d)):
        source = lax.rem(slot + 4 - k, 4)
        rows = pl.ds(pl.multiple_of(source * 64, 64), 64)
        kv[0, rows, :] = piece[0:64, :]
        kv[1, rows, :] = piece[64:128, :]
        qo[0, rows, :] = piece[128:192, :]
        qo[1, rows, :] = piece[192:256, :]
        steps[source] = piece[256:264, :].astype(f32)


def project_body(place, rows, *refs):
    blocks, (key_out, value_out) = refs[:8], refs[8:]
    for which, out in ((0, key_out), (1, value_out)):

        def tile(t, carry):
            span = pl.ds(pl.multiple_of(t * 128, 128), 128)
            total = jnp.zeros((128, 256), f32)
            for m in range(8):
                total += dot(rows[span, m * 256 : m * 256 + 256], blocks[m][which], 1, 0)
            out[span, :] = total.astype(out.dtype)
            return carry

        lax.fori_loop(0, 4, tile, 0)


def query_body(place, rows, *refs):
    blocks, (query_out, out_own, out_other) = refs[:8], refs[8:]
    z, core = place[1], place[2]

    def tile(t, carry):
        span = pl.ds(pl.multiple_of(t * 128, 128), 128)
        total = jnp.zeros((128, 256), f32)
        for m in range(8):
            total += dot(rows[span, m * 256 : m * 256 + 256], blocks[m][0], 1, 0)
        query_out[span, :] = total
        return carry

    lax.fori_loop(0, 4, tile, 0)
    for m in range(8):
        source = lax.rem(z + m, 8)
        span = pl.ds(pl.multiple_of(lax.rem(source, 4) * 256, 256), 256)
        kept = lax.div(source, 4) == core

        @pl.when(kept)
        def _():
            out_own[span, :] = blocks[m][1]

        @pl.when(jnp.logical_not(kept))
        def _():
            out_other[span, :] = blocks[m][1]


def sides(own, other, first):
    return jnp.where(first, own, other), jnp.where(first, other, own)


def normed(own, other, first, epsilon):
    low, high = sides(own, other, first)
    square = jnp.sum(low * low, axis=-1, keepdims=True) + jnp.sum(high * high, axis=-1, keepdims=True)
    factor = lax.rsqrt(square / 512 + epsilon)
    return (low * factor).astype(bf16), (high * factor).astype(bf16)


def grads_body(place, key_own, key_other, value_own, value_other, step, weights, own_out, *refs):
    outs, (keys, errors, hidden, grad_gate, grad_up, whole) = refs[:7], refs[7:]
    z, core = place[1], place[2]
    first = core == 0
    half = pl.ds(pl.multiple_of(core * 256, 256), 256)

    def tile(t, carry):
        span = pl.ds(pl.multiple_of(t * 128, 128), 128)
        low, high = normed(key_own[span, :], key_other[span, :], first, 1e-06)
        keys[span, 0:256] = low
        keys[span, 256:512] = high
        scale = step[span, :]
        low, high = sides(value_own[span, :], value_other[span, :], first)
        errors[span, 0:256] = (-(scale * low.astype(f32))).astype(bf16)
        errors[span, 256:512] = (-(scale * high.astype(f32))).astype(bf16)
        k = keys[span, :]
        gate = dot(k, weights[0, :, half], 1, 0)
        up = dot(k, weights[1, :, half], 1, 0)
        back = dot(errors[span, :], weights[2, :, half], 1, 0)
        squash = jax.nn.sigmoid(gate)
        hidden[span, :] = (gate * squash * up).astype(bf16)
        grad_gate[span, :] = (back * up * squash * (1.0 + gate * (1.0 - squash))).astype(bf16)
        grad_up[span, :] = (back * gate * squash).astype(bf16)
        return carry

    lax.fori_loop(0, 4, tile, 0)
    whole[0] = dot(keys[...], grad_gate[...], 0, 0)
    whole[1] = dot(keys[...], grad_up[...], 0, 0)
    whole[2] = dot(errors[...], hidden[...], 0, 0)
    for m in range(8):
        span = pl.ds(pl.multiple_of(lax.rem(z + m, 8) * 64, 64), 64)
        for i in range(3):
            if m == 0:
                own_out[i * 64 : i * 64 + 64, :] = whole[i, span, :]
            else:
                outs[m - 1][i * 64 : i * 64 + 64, :] = whole[i, span, :].astype(bf16)


def order_body(place, *refs):
    for m in range(8):
        span = pl.ds(pl.multiple_of(lax.rem(place[1] + m, 8) * 64, 64), 64)
        for i in range(3):
            refs[8][i, span, :] = refs[m][i * 64 : i * 64 + 64, :]


def newton_body(place, own, other, weights, rate, out, x_ref):
    first = place[2] == 0

    def matrix(m, carry):
        low, high = sides(own[m], other[m], first)
        low, high = low.astype(f32), high.astype(f32)
        norm = jnp.sqrt(jnp.sum(low * low) + jnp.sum(high * high)) + 1e-06
        x_ref[:, 0:256] = (low / norm).astype(bf16)
        x_ref[:, 256:512] = (high / norm).astype(bf16)
        for _ in range(NS_ITERS):
            x = x_ref[...]
            gram = dot(x, x, 0, 0).astype(bf16)
            cubic = dot(x, gram, 1, 0)
            quintic = dot(cubic.astype(bf16), gram, 1, 0)
            x_ref[...] = (
                coef_linear * x.astype(f32) + coef_cubic * cubic + coef_quintic * quintic
            ).astype(bf16)
        out[m] = (weights[m].astype(f32) - rate[0, 0] * x_ref[...].astype(f32)).astype(bf16)
        return carry

    lax.fori_loop(0, 3, matrix, 0)


def apply_body(place, query_own, query_other, updated, out_own, out_other, own, low, high, top, bottom):
    first = place[2] == 0

    def tile(t, carry):
        span = pl.ds(pl.multiple_of(t * 128, 128), 128)
        query = jnp.concatenate(normed(query_own[span, :], query_other[span, :], first, 1e-06), axis=1)
        gate = dot(query, updated[0], 1, 0)
        up = dot(query, updated[1], 1, 0)
        hid = (gate * jax.nn.sigmoid(gate) * up).astype(bf16)
        mixed = dot(hid, updated[2], 1, 1)
        mixed = mixed * lax.rsqrt(jnp.mean(mixed * mixed, axis=-1, keepdims=True) + 1e-05)
        left, right = sides(mixed[:, 0:256], mixed[:, 256:512], first)
        done = dot(left.astype(bf16), out_own[...], 1, 1) + dot(right.astype(bf16), out_other[...], 1, 1)
        for which, out in ((0, own), (1, low), (2, high)):

            @pl.when(t == which)
            def _():
                out[...] = done

        @pl.when(t == 3)
        def _():
            top[...] = done[0:64].astype(bf16)
            bottom[...] = done[64:128].astype(bf16)

        return carry

    lax.fori_loop(0, 4, tile, 0)


def relay_body(place, low, high, top, bottom, low_out, high_out):
    high_out[0:64, :] = (high[0:64, :] + top[...].astype(f32)).astype(bf16)
    high_out[64:128, :] = high[64:128, :].astype(bf16)
    low_out[0:64, :] = low[0:64, :].astype(bf16)
    low_out[64:128, :] = (low[64:128, :] + bottom[...].astype(f32)).astype(bf16)


def to_head_chips(pieces):
    got = []
    for k, part in enumerate(pieces):
        pairs = []
        for source in range(4):
            for c in range(2):
                j = (source + k) % 4
                pairs.append((source * 2 + c, (2 * c + j // 2) * 2 + j % 2))
        got.append(lax.ppermute(part, ("y", "head"), pairs))
    return got


def ring_gather(chunk, ups, downs):
    up, down = [chunk], [chunk]
    for step in range(4):
        if step < ups:
            up.append(moved(up[-1], "z", 1))
        if step < downs:
            down.append(moved(down[-1], "z", -1))
    return down + up[:0:-1]


def shards(group_in, w_qkv, w_out, step_sizes, fast_weights, momentum, momentum_decay, fast_rate):
    core, y, z = lax.axis_index("head"), lax.axis_index("y"), lax.axis_index("z")
    owner = (y // 2) == core
    place = jnp.stack([y, z, core])
    tokens = group_in[0]

    steps = step_sizes[0].T
    steps_high = lax.reduce_precision(steps, 8, 7)
    extra = jnp.concatenate([steps_high, steps - steps_high], axis=1).astype(bf16)
    extra = jnp.broadcast_to(extra[:, None, :], (2, 8, 256))
    pieces = kernel_call(
        pack_body, "pack", [shape(264, 256)] * 4, [place, w_qkv[0], w_out[0].T, extra]
    )
    got = to_head_chips(pieces)

    turned = lax.dynamic_slice_in_dim(jnp.concatenate([tokens, tokens], axis=1), z * 256, 2048, 1)
    from_low = moved(turned, "y", 1)
    from_high = moved(turned, "y", -1)
    far = [moved(from_low[:64], "y", 1), moved(from_high[64:], "y", -1)]

    key_value, query_out, step_rows = kernel_call(
        sort_body,
        "sort",
        [shape(2, 256, 256), shape(2, 256, 256), shape(4, 8, 256, dtype=f32)],
        [place, *got],
    )
    step_all = step_rows[:, 0, :128] + step_rows[:, 0, 128:]
    step = jnp.concatenate(
        [lax.dynamic_index_in_dim(step_all, (y + k) % 4, 0, False) for k in (0, 3, 1, 2)]
    )[:, None]

    pairs = [(yy * 2 + yy // 2, yy * 2 + 1 - yy // 2) for yy in range(4)]
    mine = lax.dynamic_index_in_dim(fast_weights[0], y % 2, 0, False)
    weights = jnp.where(owner, mine, lax.ppermute(mine, ("y", "head"), pairs))
    local_momentum = lax.dynamic_index_in_dim(momentum[0], y % 2, 0, False)
    scalars = jnp.stack(
        [
            lax.dynamic_index_in_dim(momentum_decay[0], y % 2, 0, False),
            lax.dynamic_index_in_dim(fast_rate[0], y % 2, 0, False),
        ]
    )

    def momentum_part(half):
        part = lax.dynamic_slice(local_momentum, (0, z * 64, half * 256), (3, 64, 256))
        return part.astype(f32).reshape(192, 256)

    payload = jnp.concatenate(
        [momentum_part(1 - core), jnp.broadcast_to(jnp.repeat(scalars, 128), (8, 256))], axis=0
    )
    payload = lax.ppermute(payload, ("y", "head"), pairs)
    momentum_own = jnp.where(owner, momentum_part(core), payload[:192])
    decay = jnp.where(owner, scalars[0], payload[192, 0])
    rate = jnp.where(owner, scalars[1], payload[192, 128]).reshape(1, 1)

    rows = jnp.concatenate([turned, from_low, from_high, *far], axis=0)
    key_half, value_half = kernel_call(
        project_body,
        "project",
        [shape(512, 256, dtype=f32), shape(512, 256)],
        [place, rows, *ring_gather(key_value, 4, 3)],
        flops=2 * 512 * 2048 * 512,
    )
    step, weights, momentum_own = lax.optimization_barrier((step, weights, momentum_own))
    key_other, value_other = swapped(key_half), swapped(value_half)
    own_sum, *parts = kernel_call(
        grads_body,
        "grads",
        [shape(192, 256, dtype=f32)] + [shape(192, 256)] * 7,
        [place, key_half, key_other, value_half, value_other, step, weights],
        flops=2 * 512 * 512 * 256 * 6,
        scratch=[
            pltpu.VMEM((512, 512), bf16),
            pltpu.VMEM((512, 512), bf16),
            pltpu.VMEM((512, 256), bf16),
            pltpu.VMEM((512, 256), bf16),
            pltpu.VMEM((512, 256), bf16),
            pltpu.VMEM((3, 512, 256), f32),
        ],
    )
    order = (4, 3, 5, 2, 6, 1, 7)
    total = own_sum
    for m in order:
        total = total + moved(parts[m - 1], "z", m).astype(f32)
    moment = (decay * momentum_own + total).astype(bf16)
    around = {m: moved(moment, "z", 8 - m) for m in order}
    around[0] = moment
    moment_half = kernel_call(
        order_body, "order", shape(3, 512, 256), [place] + [around[m] for m in range(8)]
    )
    moment_other = swapped(moment_half)

    query_half, out_own, out_sent = kernel_call(
        query_body,
        "query",
        [shape(512, 256, dtype=f32), shape(1024, 256), shape(1024, 256)],
        [place, rows, *ring_gather(query_out, 3, 4)],
        flops=2 * 512 * 2048 * 256,
    )
    query_other, out_other = swapped(query_half), swapped(out_sent)

    made = kernel_call(
        newton_body,
        "newton",
        shape(3, 512, 512),
        [place, moment_half, moment_other, weights, rate],
        flops=2 * 512**3 * 18,
        scratch=[pltpu.VMEM((512, 512), bf16)],
        limit=32,
    )
    blocks = shape(128, 1024, dtype=f32)
    own, low, high, top, bottom = kernel_call(
        apply_body,
        "apply",
        [blocks, blocks, blocks, shape(64, 1024), shape(64, 1024)],
        [place, query_half, query_other, made, out_own, out_other],
        flops=2 * 512**3 * 5,
        limit=32,
    )
    low, high = kernel_call(
        relay_body,
        "relay",
        [shape(128, 1024)] * 2,
        [place, low, high, moved(top, "y", 1), moved(bottom, "y", -1)],
    )
    sent_low, sent_high = moved(low, "y", -1), moved(high, "y", 1)
    own_tokens = lax.dynamic_slice_in_dim(tokens, core * 1024, 1024, 1)
    layer_out = (
        own_tokens.astype(f32) + own + sent_low.astype(f32) + sent_high.astype(f32)
    ).astype(bf16)
    handed = moved(layer_out[None], "section", 1)

    def along(value, hops):
        return lax.ppermute(
            value, ("y", "head"), [(a * 2 + c, b * 2 + c) for c in range(2) for a, b in hops(2 * c)]
        )

    def outer(a):
        return [(a, (a + 3) % 4), (a + 1, (a + 2) % 4)]

    made, _ = lax.optimization_barrier((made, top))
    across = along(made, lambda a: [(a, a + 1), (a + 1, a)])
    outward = along(made, outer)
    relayed = along(across[:, :256], outer)
    traded = along(outward[:, 256:], lambda a: [((a + 3) % 4, (a + 2) % 4), ((a + 2) % 4, (a + 3) % 4)])
    odd = (y % 2) == 1
    near = jnp.where(owner, made, outward)
    beyond = jnp.where(owner, across, jnp.concatenate([relayed, traded], axis=1))
    swap = jnp.where(owner, odd, jnp.logical_not(odd))
    fast_next = jnp.stack([jnp.where(swap, beyond, near), jnp.where(swap, near, beyond)])
    return (handed, fast_next[None])


def solution(mesh):
    torus = Mesh(
        mesh.devices.reshape(mesh.shape["section"], 8, 4, mesh.shape["head"]),
        ("section", "z", "y", "head"),
    )
    return jax.shard_map(
        shards,
        mesh=torus,
        in_specs=(
            P("section", TOK, None),
            P("section", None, TOK, "head"),
            P("section", "head", TOK),
            P("section", TOK, "head"),
            P("section", "head", None, None, None),
            P("section", "head", None, None, None),
            P("section", "head"),
            P("section", "head"),
        ),
        out_specs=(P("section", TOK, "head"), P("section", "head", None, None, None)),
        check_vma=False,
    )
```

```python
import jax
import jax.numpy as jnp
from jax import lax
from jax.experimental import pallas as pl
from jax.experimental.pallas import tpu as pltpu
from jax.sharding import Mesh
from jax.sharding import PartitionSpec as P

NS_ITERS = 2
TOK = ("z", "y")

coef_linear = 3.4445
coef_cubic = -4.775
coef_quintic = 2.0315

bf16 = jnp.bfloat16
f32 = jnp.float32


def moved(value, axis, steps):
    count = lax.axis_size(axis)
    return lax.ppermute(value, axis, [(i, (i + steps) % count) for i in range(count)])


def swapped(value):
    return lax.ppermute(value, "head", [(0, 1), (1, 0)])


def dot(a, b, ca, cb):
    return lax.dot_general(a, b, (((ca,), (cb,)), ((), ())), preferred_element_type=f32)


def kernel_call(body, name, outs, args, flops=0, scratch=(), limit=24):
    size = sum(a.size * a.dtype.itemsize for a in args[1:])
    return pl.pallas_call(
        body,
        name=name,
        out_shape=outs,
        in_specs=[pl.BlockSpec(memory_space=pltpu.SMEM)]
        + [pl.BlockSpec(memory_space=pltpu.VMEM)] * (len(args) - 1),
        out_specs=jax.tree.map(lambda _: pl.BlockSpec(memory_space=pltpu.VMEM), outs),
        scratch_shapes=list(scratch),
        compiler_params=pltpu.CompilerParams(vmem_limit_bytes=limit << 20),
        cost_estimate=pl.CostEstimate(flops=flops, bytes_accessed=size, transcendentals=0),
    )(*args)


def shape(*dims, dtype=bf16):
    return jax.ShapeDtypeStruct(dims, dtype)


def pack_body(place, w_ref, o_ref, extra_ref, *outs):
    y = place[0]
    for k, out in enumerate(outs):
        j = lax.rem(y + k, 4)
        columns = pl.ds(pl.multiple_of(j * 256, 256), 256)
        for row, component in enumerate((1, 2, 0)):
            out[row * 64 : row * 64 + 64, :] = w_ref[component, :, columns]
        out[192:256, :] = o_ref[:, columns]
        out[256:264, :] = extra_ref[lax.div(j, 2)]


def sort_body(place, a, b, c, d, chunk, steps):
    slot = 2 * lax.rem(place[0], 2) + place[2]
    for k, piece in enumerate((a, b, c, d)):
        source = lax.rem(slot + 4 - k, 4)
        rows = pl.ds(pl.multiple_of(source * 64, 64), 64)
        for i in range(4):
            chunk[i, rows, :] = piece[i * 64 : i * 64 + 64, :]
        steps[source] = piece[256:264, :].astype(f32)


def project_body(place, rows, *refs):
    blocks, out, stack = refs[:8], refs[8], refs[9]
    for which in range(2):
        for m in range(8):
            stack[m * 256 : m * 256 + 256, :] = blocks[m][which]
        out[which * 512 : which * 512 + 512, :] = dot(rows[...], stack[...], 1, 0)


def query_body(place, rows, *refs):
    blocks, (query_out, out_own, sent, stack) = refs[:8], refs[8:]
    z, core = place[1], place[2]
    for m in range(8):
        stack[m * 256 : m * 256 + 256, :] = blocks[m][0 if m == 4 else 2]
    query_out[...] = dot(rows[...], stack[...], 1, 0)

    def split(t, carry):
        span = pl.ds(pl.multiple_of(t * 128, 128), 128)
        value = query_out[span, :]
        coarse = value.astype(bf16)
        sent[span, :] = coarse
        sent[pl.ds(pl.multiple_of(t * 128 + 512, 128), 128), :] = (value - coarse.astype(f32)).astype(bf16)
        return carry

    lax.fori_loop(0, 4, split, 0)
    for m in range(8):
        source = lax.rem(z + m, 8)
        start = lax.rem(source, 4) * 256
        kept = lax.div(source, 4) == core

        @pl.when(kept)
        def _():
            out_own[pl.ds(pl.multiple_of(start, 256), 256), :] = blocks[m][1 if m == 4 else 3]

        @pl.when(jnp.logical_not(kept))
        def _():
            sent[pl.ds(pl.multiple_of(start + 1024, 256), 256), :] = blocks[m][1 if m == 4 else 3]


def sides(own, other, first):
    return jnp.where(first, own, other), jnp.where(first, other, own)


def normed(own, other, first, epsilon):
    low, high = sides(own, other, first)
    square = jnp.sum(low * low, axis=-1, keepdims=True) + jnp.sum(high * high, axis=-1, keepdims=True)
    factor = lax.rsqrt(square / 512 + epsilon)
    return (low * factor).astype(bf16), (high * factor).astype(bf16)


def grads_body(place, pair_own, pair_other, step, weights, own_out, *refs):
    outs, (keys, errors, hidden, grad_gate, grad_up, gate_ref, up_ref, back_ref, whole) = refs[:7], refs[7:]
    z, core = place[1], place[2]
    first = core == 0
    half = pl.ds(pl.multiple_of(core * 256, 256), 256)

    def inputs(t, carry):
        span = pl.ds(pl.multiple_of(t * 128, 128), 128)
        low, high = normed(pair_own[span, :], pair_other[span, :], first, 1e-06)
        keys[span, 0:256] = low
        keys[span, 256:512] = high
        scale = step[span, :]
        down = pl.ds(pl.multiple_of(t * 128 + 512, 128), 128)
        low, high = sides(pair_own[down, :], pair_other[down, :], first)
        errors[span, 0:256] = (-(scale * low.astype(bf16).astype(f32))).astype(bf16)
        errors[span, 256:512] = (-(scale * high.astype(bf16).astype(f32))).astype(bf16)
        return carry

    lax.fori_loop(0, 4, inputs, 0)
    gate_ref[...] = dot(keys[...], weights[0, :, half], 1, 0)
    up_ref[...] = dot(keys[...], weights[1, :, half], 1, 0)
    back_ref[...] = dot(errors[...], weights[2, :, half], 1, 0)

    def middle(t, carry):
        span = pl.ds(pl.multiple_of(t * 128, 128), 128)
        gate, up, back = gate_ref[span, :], up_ref[span, :], back_ref[span, :]
        squash = jax.nn.sigmoid(gate)
        hidden[span, :] = (gate * squash * up).astype(bf16)
        grad_gate[span, :] = (back * up * squash * (1.0 + gate * (1.0 - squash))).astype(bf16)
        grad_up[span, :] = (back * gate * squash).astype(bf16)
        return carry

    lax.fori_loop(0, 4, middle, 0)
    whole[0] = dot(keys[...], grad_gate[...], 0, 0)
    whole[1] = dot(keys[...], grad_up[...], 0, 0)
    whole[2] = dot(errors[...], hidden[...], 0, 0)
    for m in range(8):
        span = pl.ds(pl.multiple_of(lax.rem(z + m, 8) * 64, 64), 64)
        for i in range(3):
            if m == 0:
                own_out[i * 64 : i * 64 + 64, :] = whole[i, span, :]
            else:
                outs[m - 1][i * 64 : i * 64 + 64, :] = whole[i, span, :].astype(bf16)


def order_body(place, *refs):
    for m in range(8):
        span = pl.ds(pl.multiple_of(lax.rem(place[1] + m, 8) * 64, 64), 64)
        for i in range(3):
            refs[8][i, span, :] = refs[m][i * 64 : i * 64 + 64, :]


def newton_body(place, own, other, weights, rate, out, x_ref):
    first = place[2] == 0

    def matrix(m, carry):
        low, high = sides(own[m], other[m], first)
        low, high = low.astype(f32), high.astype(f32)
        norm = jnp.sqrt(jnp.sum(low * low) + jnp.sum(high * high)) + 1e-06
        x_ref[:, 0:256] = (low / norm).astype(bf16)
        x_ref[:, 256:512] = (high / norm).astype(bf16)
        for _ in range(NS_ITERS):
            x = x_ref[...]
            gram = dot(x, x, 0, 0).astype(bf16)
            cubic = dot(x, gram, 1, 0)
            quintic = dot(cubic.astype(bf16), gram, 1, 0)
            x_ref[...] = (
                coef_linear * x.astype(f32) + coef_cubic * cubic + coef_quintic * quintic
            ).astype(bf16)
        out[m] = (weights[m].astype(f32) - rate[0, 0] * x_ref[...].astype(f32)).astype(bf16)
        return carry

    lax.fori_loop(0, 3, matrix, 0)


def apply_body(place, query_own, out_own, other, updated, out, top, bottom, *refs):
    query, gate_ref, up_ref, hidden, mixed, left_ref, right_ref, full = refs
    first = place[2] == 0

    def spans(t):
        return pl.ds(pl.multiple_of(t * 128, 128), 128)

    def inputs(t, carry):
        span = spans(t)
        arrived = other[span, :].astype(f32) + other[spans(t + 4), :].astype(f32)
        low, high = normed(query_own[span, :], arrived, first, 1e-06)
        query[span, 0:256] = low
        query[span, 256:512] = high
        return carry

    lax.fori_loop(0, 4, inputs, 0)
    gate_ref[...] = dot(query[...], updated[0], 1, 0)
    up_ref[...] = dot(query[...], updated[1], 1, 0)

    def middle(t, carry):
        gate = gate_ref[spans(t), :]
        hidden[spans(t), :] = (gate * jax.nn.sigmoid(gate) * up_ref[spans(t), :]).astype(bf16)
        return carry

    lax.fori_loop(0, 4, middle, 0)
    mixed[...] = dot(hidden[...], updated[2], 1, 1)

    def scaled(t, carry):
        value = mixed[spans(t), :]
        value = value * lax.rsqrt(jnp.mean(value * value, axis=-1, keepdims=True) + 1e-05)
        left, right = sides(value[:, 0:256], value[:, 256:512], first)
        left_ref[spans(t), :] = left.astype(bf16)
        right_ref[spans(t), :] = right.astype(bf16)
        return carry

    lax.fori_loop(0, 4, scaled, 0)
    full[...] = dot(left_ref[...], out_own[...], 1, 1) + dot(right_ref[...], other[1024:2048, :], 1, 1)
    out[...] = full[0:384, :]
    top[...] = full[384:448, :].astype(bf16)
    bottom[...] = full[448:512, :].astype(bf16)


def relay_body(place, partial, top, bottom, low_out, high_out):
    low_out[0:64, :] = partial[128:192, :].astype(bf16)
    low_out[64:128, :] = (partial[192:256, :] + bottom[...].astype(f32)).astype(bf16)
    high_out[0:64, :] = (partial[256:320, :] + top[...].astype(f32)).astype(bf16)
    high_out[64:128, :] = partial[320:384, :].astype(bf16)


def payload_body(place, weights, momentum, scalars, out):
    out[0:1536, :] = weights[lax.rem(place[0], 2)].reshape(1536, 512)
    out[1536:1728, :] = momentum[...]
    out[1728:1736, :] = scalars[...]


def choose_body(place, mine, arrived, weights_out, momentum_out, scalars_out):
    owner = lax.div(place[0], 2) == place[2]
    columns = pl.ds(pl.multiple_of(place[2] * 256, 256), 256)

    def take(source):
        weights_out[...] = source[0:1536, :].reshape(3, 512, 512)
        momentum_out[...] = source[1536:1728, columns].astype(f32)
        scalars_out[...] = source[1728:1736, :].astype(f32)

    @pl.when(owner)
    def _():
        take(mine)

    @pl.when(jnp.logical_not(owner))
    def _():
        take(arrived)


def copies(moves, sems):
    started = [pltpu.make_async_copy(a, b, sems.at[i]) for i, (a, b) in enumerate(moves)]
    for copy in started:
        copy.start()
    for copy in started:
        copy.wait()


def emit_body(place, made, across, outward, out, sems):
    slot = lax.rem(place[0], 2)
    owner = lax.div(place[0], 2) == place[2]

    @pl.when(owner)
    def _():
        copies([(made, out.at[slot]), (across, out.at[1 - slot])], sems)

    @pl.when(jnp.logical_not(owner))
    def _():
        copies([(outward, out.at[1 - slot])], sems)


def finish_body(place, relayed, traded, _, out, sems):
    slot = lax.rem(place[0], 2)

    @pl.when(lax.div(place[0], 2) != place[2])
    def _():
        moves = [
            (relayed, out.at[slot, :, pl.ds(0, 256)]),
            (traded, out.at[slot, :, pl.ds(256, 256)]),
        ]
        copies(moves, sems)


def to_head_chips(pieces):
    got = []
    for k, part in enumerate(pieces):
        pairs = []
        for source in range(4):
            for c in range(2):
                j = (source + k) % 4
                pairs.append((source * 2 + c, (2 * c + j // 2) * 2 + j % 2))
        got.append(lax.ppermute(part, ("y", "head"), pairs))
    return got


def shards(group_in, w_qkv, w_out, step_sizes, fast_weights, momentum, momentum_decay, fast_rate):
    core, y, z = lax.axis_index("head"), lax.axis_index("y"), lax.axis_index("z")
    place = jnp.stack([y, z, core])

    steps = step_sizes[0].T
    steps_high = lax.reduce_precision(steps, 8, 7)
    extra = jnp.concatenate([steps_high, steps - steps_high], axis=1).astype(bf16)
    extra = jnp.broadcast_to(extra[:, None, :], (2, 8, 256))
    pieces = kernel_call(
        pack_body, "pack", [shape(264, 256)] * 4, [place, w_qkv[0], w_out[0].T, extra]
    )
    chunk, step_rows = kernel_call(
        sort_body,
        "sort",
        [shape(4, 256, 256), shape(4, 8, 256, dtype=f32)],
        [place, *to_head_chips(pieces)],
    )

    up, down = [chunk], [chunk]
    for _ in range(3):
        up.append(moved(up[-1], "z", 1))
        down.append(moved(down[-1], "z", -1))
    key_value_far = moved(up[3][0:2], "z", 1)
    query_out_far = moved(down[3][2:4], "z", -1)

    step_all = step_rows[:, 0, :128] + step_rows[:, 0, 128:]
    step = jnp.concatenate(
        [lax.dynamic_index_in_dim(step_all, (y + k) % 4, 0, False) for k in (0, 3, 1, 2)]
    )[:, None]

    tokens, _ = lax.optimization_barrier((group_in[0], chunk))
    turned = lax.dynamic_slice_in_dim(jnp.concatenate([tokens, tokens], axis=1), z * 256, 2048, 1)
    rows = jnp.concatenate([turned, moved(turned, "y", 1), moved(turned, "y", -1), moved(turned, "y", 2)])

    part = lax.dynamic_slice(momentum[0], (y % 2, 0, z * 64, 0), (1, 3, 64, 512)).reshape(192, 512)
    scalars = jnp.stack([momentum_decay[0], fast_rate[0]])
    scalars = lax.dynamic_index_in_dim(scalars, y % 2, 1, False)
    terms = []
    for _ in range(3):
        term = lax.reduce_precision(scalars, 8, 7)
        terms.append(term)
        scalars = scalars - term
    terms = jnp.pad(jnp.concatenate(terms), (0, 2))
    terms = jnp.broadcast_to(terms[:, None], (8, 512)).astype(bf16)
    part, terms, _ = lax.optimization_barrier((part, terms, chunk))
    mine = kernel_call(
        payload_body, "payload", shape(1736, 512), [place, fast_weights[0], part, terms]
    )
    pairs = [(yy * 2 + yy // 2, yy * 2 + 1 - yy // 2) for yy in range(4)]
    weights, momentum_own, terms = kernel_call(
        choose_body,
        "choose",
        [shape(3, 512, 512), shape(192, 256, dtype=f32), shape(8, 512, dtype=f32)],
        [place, mine, lax.ppermute(mine, ("y", "head"), pairs)],
    )
    decay = terms[0, 0] + terms[2, 0] + terms[4, 0]
    rate = (terms[1, 0] + terms[3, 0] + terms[5, 0]).reshape(1, 1)

    pair = kernel_call(
        project_body,
        "project",
        shape(1024, 256, dtype=f32),
        [place, rows, *down, key_value_far, *up[:0:-1]],
        flops=2 * 512 * 2048 * 512,
        scratch=[pltpu.VMEM((2048, 256), bf16)],
    )
    step, weights, momentum_own, pair = lax.optimization_barrier((step, weights, momentum_own, pair))
    own_sum, *parts = kernel_call(
        grads_body,
        "grads",
        [shape(192, 256, dtype=f32)] + [shape(192, 256)] * 7,
        [place, pair, swapped(pair), step, weights],
        flops=2 * 512 * 512 * 256 * 6,
        scratch=[pltpu.VMEM((512, 512), bf16)] * 2
        + [pltpu.VMEM((512, 256), bf16)] * 3
        + [pltpu.VMEM((512, 256), f32)] * 3
        + [pltpu.VMEM((3, 512, 256), f32)],
    )
    to_up = moved(parts[3 - 1], "z", 1)
    to_far = moved(parts[4 - 1], "z", 2)
    to_down = moved(parts[5 - 1], "z", -1)
    near = [moved(parts[1 - 1], "z", 1), moved(parts[7 - 1], "z", -1)]
    ahead = (parts[2 - 1].astype(f32) + to_up.astype(f32) + to_far.astype(f32)).astype(bf16)
    behind = (parts[6 - 1].astype(f32) + to_down.astype(f32)).astype(bf16)
    rows, _ = lax.optimization_barrier((rows, parts[3]))
    query_half, out_own, sent = kernel_call(
        query_body,
        "query",
        [shape(512, 256, dtype=f32), shape(1024, 256), shape(2048, 256)],
        [place, rows, *down, query_out_far, *up[:0:-1]],
        flops=2 * 512 * 2048 * 256,
        scratch=[pltpu.VMEM((2048, 256), bf16)],
    )
    arrived = swapped(sent)
    own_sum, _ = lax.optimization_barrier((own_sum, sent))
    total = own_sum
    for term in (*near, moved(ahead, "z", 2), moved(behind, "z", -2)):
        total = total + term.astype(f32)
    moment = (decay * momentum_own + total).astype(bf16)
    around = {0: moment, 2: moved(moment, "z", -2), 6: moved(moment, "z", 2)}
    around[1], around[7] = moved(moment, "z", -1), moved(moment, "z", 1)
    around[3], around[5] = moved(around[2], "z", -1), moved(around[6], "z", 1)
    around[4] = moved(around[2], "z", -2)
    moment_half = kernel_call(
        order_body, "order", shape(3, 512, 256), [place] + [around[m] for m in range(8)]
    )

    moment_other = swapped(moment_half)
    moment_half, arrived = lax.optimization_barrier((moment_half, arrived))
    made = kernel_call(
        newton_body,
        "newton",
        shape(3, 512, 512),
        [place, moment_half, moment_other, weights, rate],
        flops=2 * 512**3 * 18,
        scratch=[pltpu.VMEM((512, 512), bf16)],
    )

    def along(value, hops):
        return lax.ppermute(
            value, ("y", "head"), [(a * 2 + c, b * 2 + c) for c in range(2) for a, b in hops(2 * c)]
        )

    def outer(a):
        return [(a, (a + 3) % 4), (a + 1, (a + 2) % 4)]

    across = along(made, lambda a: [(a, a + 1), (a + 1, a)])
    outward = along(made, outer)

    partial, top, bottom = kernel_call(
        apply_body,
        "apply",
        [shape(384, 1024, dtype=f32), shape(64, 1024), shape(64, 1024)],
        [place, query_half, out_own, arrived, made],
        flops=2 * 512**3 * 5,
        scratch=[
            pltpu.VMEM((512, 512), bf16),
            pltpu.VMEM((512, 512), f32),
            pltpu.VMEM((512, 512), f32),
            pltpu.VMEM((512, 512), bf16),
            pltpu.VMEM((512, 512), f32),
            pltpu.VMEM((512, 256), bf16),
            pltpu.VMEM((512, 256), bf16),
            pltpu.VMEM((512, 1024), f32),
        ],
    )
    low, high = kernel_call(
        relay_body,
        "relay",
        [shape(128, 1024)] * 2,
        [place, partial, moved(top, "y", 1), moved(bottom, "y", -1)],
    )
    across, outward, _ = lax.optimization_barrier((across, outward, low))
    relayed = along(across[:, :256], outer)
    traded = along(outward[:, 256:], lambda a: [((a + 3) % 4, (a + 2) % 4), ((a + 2) % 4, (a + 3) % 4)])

    def emit(body, name, values, **more):
        count = len(values)
        return pl.pallas_call(
            body,
            name=name,
            out_shape=shape(2, 3, 512, 512),
            in_specs=[pl.BlockSpec(memory_space=pltpu.SMEM)]
            + [pl.BlockSpec(memory_space=pltpu.VMEM)] * count
            + [pl.BlockSpec(memory_space=pl.ANY)] * (len(more) > 0),
            out_specs=pl.BlockSpec(memory_space=pl.ANY),
            scratch_shapes=[pltpu.SemaphoreType.DMA((2,))],
            compiler_params=pltpu.CompilerParams(vmem_limit_bytes=16 << 20),
            cost_estimate=pl.CostEstimate(flops=0, bytes_accessed=3 << 20, transcendentals=0),
            **({"input_output_aliases": {count + 1: 0}} if more else {}),
        )(place, *values, *more.values())

    fast_next = emit(emit_body, "emit", (made, across, outward))
    fast_next = emit(finish_body, "finish", (relayed, traded), base=fast_next)
    sent_low, sent_high = moved(low, "y", -1), moved(high, "y", 1)
    own_tokens = lax.dynamic_slice_in_dim(group_in[0], core * 1024, 1024, 1)
    layer_out = (
        own_tokens.astype(f32) + partial[:128] + sent_low.astype(f32) + sent_high.astype(f32)
    ).astype(bf16)
    handed = moved(layer_out[None], "section", 1)
    return (handed, fast_next[None])


def solution(mesh):
    torus = Mesh(
        mesh.devices.reshape(mesh.shape["section"], 8, 4, mesh.shape["head"]),
        ("section", "z", "y", "head"),
    )
    return jax.shard_map(
        shards,
        mesh=torus,
        in_specs=(
            P("section", TOK, None),
            P("section", None, TOK, "head"),
            P("section", "head", TOK),
            P("section", TOK, "head"),
            P("section", "head", None, None, None),
            P("section", "head", None, None, None),
            P("section", "head"),
            P("section", "head"),
        ),
        out_specs=(P("section", TOK, "head"), P("section", "head", None, None, None)),
        check_vma=False,
    )
```

```python
import jax
import jax.numpy as jnp
from jax import lax
from jax.experimental import pallas as pl
from jax.experimental.pallas import tpu as pltpu
from jax.sharding import Mesh
from jax.sharding import PartitionSpec as P


NS_ITERS = 2
TOK = ("z", "y")

coef_linear = 3.4445
coef_cubic = -4.775
coef_quintic = 2.0315

bf16 = jnp.bfloat16
f32 = jnp.float32


def moved(value, axis, steps):
    count = lax.axis_size(axis)
    return lax.ppermute(value, axis, [(i, (i + steps) % count) for i in range(count)])


def swapped(value):
    return lax.ppermute(value, "head", [(0, 1), (1, 0)])


def dot(a, b, ca, cb):
    return lax.dot_general(a, b, (((ca,), (cb,)), ((), ())), preferred_element_type=f32)


def kernel_call(body, outs, args, flops=0, scratch=(), limit=24):
    size = sum(a.size * a.dtype.itemsize for a in args[1:])
    return pl.pallas_call(
        body,
        out_shape=outs,
        in_specs=[pl.BlockSpec(memory_space=pltpu.SMEM)]
        + [pl.BlockSpec(memory_space=pltpu.VMEM)] * (len(args) - 1),
        out_specs=jax.tree.map(lambda _: pl.BlockSpec(memory_space=pltpu.VMEM), outs),
        scratch_shapes=list(scratch),
        compiler_params=pltpu.CompilerParams(vmem_limit_bytes=limit << 20),
        cost_estimate=pl.CostEstimate(flops=flops, bytes_accessed=size, transcendentals=0),
    )(*args)


def shape(*dims, dtype=bf16):
    return jax.ShapeDtypeStruct(dims, dtype)


def pack_body(place, w_ref, o_ref, extra_ref, *outs):
    y = place[0]
    for k, out in enumerate(outs):
        j = lax.rem(y + k, 4)
        columns = pl.ds(pl.multiple_of(j * 256, 256), 256)
        for row, component in enumerate((1, 2, 0)):
            out[row * 64 : row * 64 + 64, :] = w_ref[component, :, columns]
        out[192:256, :] = o_ref[:, columns]
        out[256:264, :] = extra_ref[lax.div(j, 2)]


def sort_body(place, a, b, c, d, key_value, query_out, steps):
    slot = 2 * lax.rem(place[0], 2) + place[2]
    for k, piece in enumerate((a, b, c, d)):
        source = lax.rem(slot + 4 - k, 4)
        rows = pl.ds(pl.multiple_of(source * 64, 64), 64)
        for i in range(2):
            key_value[i, rows, :] = piece[i * 64 : i * 64 + 64, :]
            query_out[i, rows, :] = piece[i * 64 + 128 : i * 64 + 192, :]
        steps[source] = piece[256:264, :].astype(f32)


def project_body(place, rows, *refs):
    blocks, out, stack = refs[:8], refs[8], refs[9]

    def component(which, carry):
        for m in range(8):
            stack[m * 256 : m * 256 + 256, :] = blocks[m][which]
        out[pl.ds(pl.multiple_of(which * 512, 512), 512), :] = dot(rows[...], stack[...], 1, 0)
        return carry

    lax.fori_loop(0, 2, component, 0)


def query_body(place, rows, *refs):
    blocks, (query_out, out_own, sent, stack) = refs[:8], refs[8:]
    z, core = place[1], place[2]
    for m in range(8):
        stack[m * 256 : m * 256 + 256, :] = blocks[m][0]
    query_out[...] = dot(rows[...], stack[...], 1, 0)

    def split(t, carry):
        span = pl.ds(pl.multiple_of(t * 128, 128), 128)
        value = query_out[span, :]
        coarse = value.astype(bf16)
        sent[span, :] = coarse
        sent[pl.ds(pl.multiple_of(t * 128 + 512, 128), 128), :] = (value - coarse.astype(f32)).astype(bf16)
        return carry

    lax.fori_loop(0, 4, split, 0)
    for m in range(8):
        source = lax.rem(z + m, 8)
        start = lax.rem(source, 4) * 256
        kept = lax.div(source, 4) == core

        @pl.when(kept)
        def _():
            out_own[pl.ds(pl.multiple_of(start, 256), 256), :] = blocks[m][1]

        @pl.when(jnp.logical_not(kept))
        def _():
            sent[pl.ds(pl.multiple_of(start + 1024, 256), 256), :] = blocks[m][1]


def sides(own, other, first):
    return jnp.where(first, own, other), jnp.where(first, other, own)


def normed(own, other, first, epsilon):
    low, high = sides(own, other, first)
    square = jnp.sum(low * low, axis=-1, keepdims=True) + jnp.sum(high * high, axis=-1, keepdims=True)
    factor = lax.rsqrt(square / 512 + epsilon)
    return (low * factor).astype(bf16), (high * factor).astype(bf16)


def grads_body(place, pair_own, pair_other, step, weights, own_out, *refs):
    outs, (keys, errors, hidden, grad_pre, pre_ref, back_ref, whole) = refs[:7], refs[7:]
    z, core = place[1], place[2]
    first = core == 0
    half = pl.ds(pl.multiple_of(core * 256, 256), 256)

    def inputs(t, carry):
        span = pl.ds(pl.multiple_of(t * 128, 128), 128)
        low, high = normed(pair_own[span, :], pair_other[span, :], first, 1e-06)
        keys[span, 0:256] = low
        keys[span, 256:512] = high
        scale = step[span, :]
        down = pl.ds(pl.multiple_of(t * 128 + 512, 128), 128)
        low, high = sides(pair_own[down, :], pair_other[down, :], first)
        errors[span, 0:256] = (-(scale * low.astype(bf16).astype(f32))).astype(bf16)
        errors[span, 256:512] = (-(scale * high.astype(bf16).astype(f32))).astype(bf16)
        return carry

    lax.fori_loop(0, 4, inputs, 0)

    def inner(i, carry):
        pre_ref[i] = dot(keys[...], weights[i, :, half], 1, 0)
        return carry

    lax.fori_loop(0, 2, inner, 0)
    back_ref[...] = dot(errors[...], weights[2, :, half], 1, 0)

    def middle(t, carry):
        span = pl.ds(pl.multiple_of(t * 128, 128), 128)
        gate, up, back = pre_ref[0, span, :], pre_ref[1, span, :], back_ref[span, :]
        squash = jax.nn.sigmoid(gate)
        hidden[span, :] = (gate * squash * up).astype(bf16)
        grad_pre[0, span, :] = (back * up * squash * (1.0 + gate * (1.0 - squash))).astype(bf16)
        grad_pre[1, span, :] = (back * gate * squash).astype(bf16)
        return carry

    lax.fori_loop(0, 4, middle, 0)

    def outer(i, carry):
        whole[i] = dot(keys[...], grad_pre[i], 0, 0)
        return carry

    lax.fori_loop(0, 2, outer, 0)
    whole[2] = dot(errors[...], hidden[...], 0, 0)
    for m in range(8):
        span = pl.ds(pl.multiple_of(lax.rem(z + m, 8) * 64, 64), 64)
        for i in range(3):
            if m == 0:
                own_out[i * 64 : i * 64 + 64, :] = whole[i, span, :]
            else:
                outs[m - 1][i * 64 : i * 64 + 64, :] = whole[i, span, :].astype(bf16)


def order_body(place, *refs):
    for m in range(8):
        span = pl.ds(pl.multiple_of(lax.rem(place[1] + m, 8) * 64, 64), 64)
        for i in range(3):
            refs[8][i, span, :] = refs[m][i * 64 : i * 64 + 64, :]


def newton_body(place, own, other, weights, rate, out, x_ref):
    first = place[2] == 0

    def start(m, carry):
        low, high = sides(own[m], other[m], first)
        low, high = low.astype(f32), high.astype(f32)
        norm = jnp.sqrt(jnp.sum(low * low) + jnp.sum(high * high)) + 1e-06
        x_ref[m, :, 0:256] = (low / norm).astype(bf16)
        x_ref[m, :, 256:512] = (high / norm).astype(bf16)
        return carry

    lax.fori_loop(0, 3, start, 0)

    def iteration(i, carry):
        m = lax.rem(i, 3)
        x = x_ref[m]
        gram = dot(x, x, 0, 0).astype(bf16)
        cubic = dot(x, gram, 1, 0)
        quintic = dot(cubic.astype(bf16), gram, 1, 0)
        x_ref[m] = (
            coef_linear * x.astype(f32) + coef_cubic * cubic + coef_quintic * quintic
        ).astype(bf16)
        return carry

    lax.fori_loop(0, 3 * NS_ITERS, iteration, 0)

    def update(m, carry):
        out[m] = (weights[m].astype(f32) - rate[0, 0] * x_ref[m].astype(f32)).astype(bf16)
        return carry

    lax.fori_loop(0, 3, update, 0)


def apply_body(place, query_own, out_own, other, updated, out, top, bottom, *refs):
    query, pre_ref, hidden, mixed, left_ref, right_ref, full = refs
    first = place[2] == 0

    def spans(t):
        return pl.ds(pl.multiple_of(t * 128, 128), 128)

    def inputs(t, carry):
        span = spans(t)
        arrived = other[span, :].astype(f32) + other[spans(t + 4), :].astype(f32)
        low, high = normed(query_own[span, :], arrived, first, 1e-06)
        query[span, 0:256] = low
        query[span, 256:512] = high
        return carry

    lax.fori_loop(0, 4, inputs, 0)

    def inner(i, carry):
        pre_ref[i] = dot(query[...], updated[i], 1, 0)
        return carry

    lax.fori_loop(0, 2, inner, 0)

    def middle(t, carry):
        gate = pre_ref[0, spans(t), :]
        hidden[spans(t), :] = (gate * jax.nn.sigmoid(gate) * pre_ref[1, spans(t), :]).astype(bf16)
        return carry

    lax.fori_loop(0, 4, middle, 0)
    mixed[...] = dot(hidden[...], updated[2], 1, 1)

    def scaled(t, carry):
        value = mixed[spans(t), :]
        value = value * lax.rsqrt(jnp.mean(value * value, axis=-1, keepdims=True) + 1e-05)
        left, right = sides(value[:, 0:256], value[:, 256:512], first)
        left_ref[spans(t), :] = left.astype(bf16)
        right_ref[spans(t), :] = right.astype(bf16)
        return carry

    lax.fori_loop(0, 4, scaled, 0)
    full[...] = dot(left_ref[...], out_own[...], 1, 1) + dot(right_ref[...], other[1024:2048, :], 1, 1)
    out[...] = full[0:384, :]
    top[...] = full[384:448, :].astype(bf16)
    bottom[...] = full[448:512, :].astype(bf16)


def relay_body(place, partial, top, bottom, low_out, high_out):
    low_out[0:64, :] = partial[128:192, :].astype(bf16)
    low_out[64:128, :] = (partial[192:256, :] + bottom[...].astype(f32)).astype(bf16)
    high_out[0:64, :] = (partial[256:320, :] + top[...].astype(f32)).astype(bf16)
    high_out[64:128, :] = partial[320:384, :].astype(bf16)


def payload_body(place, weights, momentum, scalars, out):
    out[0:1536, :] = weights[lax.rem(place[0], 2)].reshape(1536, 512)
    out[1536:1728, :] = momentum[...]
    out[1728:1736, :] = scalars[...]


def choose_body(place, mine, arrived, weights_out, momentum_out, scalars_out):
    owner = lax.div(place[0], 2) == place[2]
    columns = pl.ds(pl.multiple_of(place[2] * 256, 256), 256)

    def take(source):
        weights_out[...] = source[0:1536, :].reshape(3, 512, 512)
        momentum_out[...] = source[1536:1728, columns].astype(f32)
        scalars_out[...] = source[1728:1736, :].astype(f32)

    @pl.when(owner)
    def _():
        take(mine)

    @pl.when(jnp.logical_not(owner))
    def _():
        take(arrived)


def copies(moves, sems):
    started = [pltpu.make_async_copy(a, b, sems.at[i]) for i, (a, b) in enumerate(moves)]
    for copy in started:
        copy.start()
    for copy in started:
        copy.wait()


def emit_body(place, made, near, out, sems):
    slot = lax.rem(place[0], 2)
    owner = lax.div(place[0], 2) == place[2]

    @pl.when(owner)
    def _():
        copies([(made, out.at[slot]), (near, out.at[1 - slot])], sems)

    @pl.when(jnp.logical_not(owner))
    def _():
        copies([(near, out.at[1 - slot])], sems)


def finish_body(place, relayed, traded, _, out, sems):
    slot = lax.rem(place[0], 2)

    @pl.when(lax.div(place[0], 2) != place[2])
    def _():
        moves = [
            (relayed, out.at[slot, :, pl.ds(0, 256)]),
            (traded, out.at[slot, :, pl.ds(256, 256)]),
        ]
        copies(moves, sems)


def to_head_chips(pieces):
    got = []
    for k, part in enumerate(pieces):
        pairs = []
        for source in range(4):
            for c in range(2):
                j = (source + k) % 4
                pairs.append((source * 2 + c, (2 * c + j // 2) * 2 + j % 2))
        got.append(lax.ppermute(part, ("y", "head"), pairs))
    return got


def ring_gather(chunk, ups, downs):
    up, down = [chunk], [chunk]
    for step in range(4):
        if step < ups:
            up.append(moved(up[-1], "z", 1))
        if step < downs:
            down.append(moved(down[-1], "z", -1))
    return down + up[:0:-1]


def section_step(group_in, w_qkv, w_out, step_sizes, fast_weights, momentum, momentum_decay, fast_rate):
    core, y, z = lax.axis_index("head"), lax.axis_index("y"), lax.axis_index("z")
    place = jnp.stack([y, z, core])

    steps = step_sizes[0].T
    steps_high = lax.reduce_precision(steps, 8, 7)
    extra = jnp.concatenate([steps_high, steps - steps_high], axis=1).astype(bf16)
    extra = jnp.broadcast_to(extra[:, None, :], (2, 8, 256))
    pieces = kernel_call(pack_body, [shape(264, 256)] * 4, [place, w_qkv[0], w_out[0].T, extra])
    key_value, query_out, step_rows = kernel_call(
        sort_body,
        [shape(2, 256, 256), shape(2, 256, 256), shape(4, 8, 256, dtype=f32)],
        [place, *to_head_chips(pieces)],
    )

    key_value_blocks = ring_gather(key_value, 4, 3)
    query_out_blocks = ring_gather(query_out, 3, 4)

    step_all = step_rows[:, 0, :128] + step_rows[:, 0, 128:]
    step = jnp.concatenate(
        [lax.dynamic_index_in_dim(step_all, (y + k) % 4, 0, False) for k in (0, 3, 1, 2)]
    )[:, None]

    tokens, _ = lax.optimization_barrier((group_in[0], pieces[0]))
    turned = lax.dynamic_slice_in_dim(jnp.concatenate([tokens, tokens], axis=1), z * 256, 2048, 1)
    rows = jnp.concatenate(
        [turned, moved(turned, "y", 1), moved(turned, "y", -1), moved(turned, "y", 2)]
    )

    part = lax.dynamic_slice(momentum[0], (y % 2, 0, z * 64, 0), (1, 3, 64, 512)).reshape(192, 512)
    scalars = jnp.stack([momentum_decay[0], fast_rate[0]])
    scalars = lax.dynamic_index_in_dim(scalars, y % 2, 1, False)
    terms = []
    for _ in range(3):
        term = lax.reduce_precision(scalars, 8, 7)
        terms.append(term)
        scalars = scalars - term
    terms = jnp.pad(jnp.concatenate(terms), (0, 2))
    terms = jnp.broadcast_to(terms[:, None], (8, 512)).astype(bf16)
    part, terms, _ = lax.optimization_barrier((part, terms, pieces[0]))
    mine = kernel_call(payload_body, shape(1736, 512), [place, fast_weights[0], part, terms])
    pairs = [(yy * 2 + yy // 2, yy * 2 + 1 - yy // 2) for yy in range(4)]
    mine_sent = lax.ppermute(mine, ("y", "head"), pairs)
    weights, momentum_own, terms = kernel_call(
        choose_body,
        [shape(3, 512, 512), shape(192, 256, dtype=f32), shape(8, 512, dtype=f32)],
        [place, mine, mine_sent],
    )
    decay = terms[0, 0] + terms[2, 0] + terms[4, 0]
    rate = (terms[1, 0] + terms[3, 0] + terms[5, 0]).reshape(1, 1)

    pair = kernel_call(
        project_body,
        shape(1024, 256, dtype=f32),
        [place, rows, *key_value_blocks],
        flops=2 * 512 * 2048 * 512,
        scratch=[pltpu.VMEM((2048, 256), bf16)],
    )
    pair_other = swapped(pair)
    own_sum, *parts = kernel_call(
        grads_body,
        [shape(192, 256, dtype=f32)] + [shape(192, 256)] * 7,
        [place, pair, pair_other, step, weights],
        flops=2 * 512 * 512 * 256 * 6,
        scratch=[pltpu.VMEM((512, 512), bf16)] * 2
        + [pltpu.VMEM((512, 256), bf16), pltpu.VMEM((2, 512, 256), bf16)]
        + [pltpu.VMEM((2, 512, 256), f32), pltpu.VMEM((512, 256), f32)]
        + [pltpu.VMEM((3, 512, 256), f32)],
    )
    to_up = moved(parts[3 - 1], "z", 1)
    to_far = moved(parts[4 - 1], "z", 2)
    to_down = moved(parts[5 - 1], "z", -1)
    near = [moved(parts[1 - 1], "z", 1), moved(parts[7 - 1], "z", -1)]
    ahead = (parts[2 - 1].astype(f32) + to_up.astype(f32) + to_far.astype(f32)).astype(bf16)
    behind = (parts[6 - 1].astype(f32) + to_down.astype(f32)).astype(bf16)
    rows, _ = lax.optimization_barrier((rows, parts[3]))
    query_half, out_own, query_sent = kernel_call(
        query_body,
        [shape(512, 256, dtype=f32), shape(1024, 256), shape(2048, 256)],
        [place, rows, *query_out_blocks],
        flops=2 * 512 * 2048 * 256,
        scratch=[pltpu.VMEM((2048, 256), bf16)],
    )
    arrived = swapped(query_sent)
    own_sum, _ = lax.optimization_barrier((own_sum, query_sent))
    total = own_sum
    for term in (*near, moved(ahead, "z", 2), moved(behind, "z", -2)):
        total = total + term.astype(f32)
    moment = (decay * momentum_own + total).astype(bf16)
    around = {0: moment, 2: moved(moment, "z", -2), 6: moved(moment, "z", 2)}
    around[1], around[7] = moved(moment, "z", -1), moved(moment, "z", 1)
    around[3], around[5] = moved(around[2], "z", -1), moved(around[6], "z", 1)
    around[4] = moved(around[2], "z", -2)
    moment_half = kernel_call(
        order_body, shape(3, 512, 256), [place] + [around[m] for m in range(8)]
    )

    moment_other = swapped(moment_half)
    moment_half, arrived = lax.optimization_barrier((moment_half, arrived))
    made = kernel_call(
        newton_body,
        shape(3, 512, 512),
        [place, moment_half, moment_other, weights, rate],
        flops=2 * 512**3 * 18,
        scratch=[pltpu.VMEM((3, 512, 512), bf16)],
    )

    def along(value, hops):
        return lax.ppermute(value, ("y", "head"), [(a * 2 + c, b * 2 + d) for a, c, b, d in hops])

    outer = [(1, 2), (0, 3), (3, 0), (2, 1)]
    near = along(
        made,
        [(a, a // 2, a ^ 1, a // 2) for a in range(4)] + [(a, 1 - a // 2, b, a // 2) for a, b in outer],
    )

    partial, top, bottom = kernel_call(
        apply_body,
        [shape(384, 1024, dtype=f32), shape(64, 1024), shape(64, 1024)],
        [place, query_half, out_own, arrived, made],
        flops=2 * 512**3 * 5,
        scratch=[
            pltpu.VMEM((512, 512), bf16),
            pltpu.VMEM((2, 512, 512), f32),
            pltpu.VMEM((512, 512), bf16),
            pltpu.VMEM((512, 512), f32),
            pltpu.VMEM((512, 256), bf16),
            pltpu.VMEM((512, 256), bf16),
            pltpu.VMEM((512, 1024), f32),
        ],
    )
    low, high = kernel_call(
        relay_body,
        [shape(128, 1024)] * 2,
        [place, partial, moved(top, "y", 1), moved(bottom, "y", -1)],
    )
    near, _ = lax.optimization_barrier((near, low))
    relayed = along(near[:, :256], [(a, a // 2, b, a // 2) for a, b in outer])
    traded = along(near[:, 256:], [(a, 1 - a // 2, a ^ 1, 1 - a // 2) for a in range(4)])

    def emit(body, values, **more):
        count = len(values)
        return pl.pallas_call(
            body,
            out_shape=shape(2, 3, 512, 512),
            in_specs=[pl.BlockSpec(memory_space=pltpu.SMEM)]
            + [pl.BlockSpec(memory_space=pltpu.VMEM)] * count
            + [pl.BlockSpec(memory_space=pl.ANY)] * (len(more) > 0),
            out_specs=pl.BlockSpec(memory_space=pl.ANY),
            scratch_shapes=[pltpu.SemaphoreType.DMA((2,))],
            compiler_params=pltpu.CompilerParams(vmem_limit_bytes=16 << 20),
            cost_estimate=pl.CostEstimate(flops=0, bytes_accessed=3 << 20, transcendentals=0),
            **({"input_output_aliases": {count + 1: 0}} if more else {}),
        )(place, *values, *more.values())

    fast_next = emit(emit_body, (made, near))
    fast_next = emit(finish_body, (relayed, traded), base=fast_next)
    sent_low, sent_high = moved(low, "y", -1), moved(high, "y", 1)
    own_tokens = lax.dynamic_slice_in_dim(group_in[0], core * 1024, 1024, 1)
    layer_out = (
        own_tokens.astype(f32) + partial[:128] + sent_low.astype(f32) + sent_high.astype(f32)
    ).astype(bf16)
    handed = moved(layer_out[None], "section", 1)
    return (handed, fast_next[None])


def solution(mesh):
    torus = Mesh(
        mesh.devices.reshape(mesh.shape["section"], 8, 4, mesh.shape["head"]),
        ("section", "z", "y", "head"),
    )
    return jax.shard_map(
        section_step,
        mesh=torus,
        in_specs=(
            P("section", TOK, None),
            P("section", None, TOK, "head"),
            P("section", "head", TOK),
            P("section", TOK, "head"),
            P("section", "head", None, None, None),
            P("section", "head", None, None, None),
            P("section", "head"),
            P("section", "head"),
        ),
        out_specs=(P("section", TOK, "head"), P("section", "head", None, None, None)),
        check_vma=False,
    )
```

```python
import jax
import jax.numpy as jnp
from jax import lax
from jax.experimental import pallas as pl
from jax.experimental.pallas import tpu as pltpu
from jax.sharding import Mesh
from jax.sharding import PartitionSpec as P


NS_ITERS = 2
TOK = ("z", "y")

coef_linear = 3.4445
coef_cubic = -4.775
coef_quintic = 2.0315

bf16 = jnp.bfloat16
f32 = jnp.float32


def moved(value, axis, steps):
    count = lax.axis_size(axis)
    return lax.ppermute(value, axis, [(i, (i + steps) % count) for i in range(count)])


def swapped(value):
    return lax.ppermute(value, "head", [(0, 1), (1, 0)])


def dot(a, b, ca, cb):
    return lax.dot_general(a, b, (((ca,), (cb,)), ((), ())), preferred_element_type=f32)


def kernel_call(body, outs, args, flops=0, scratch=(), limit=24):
    size = sum(a.size * a.dtype.itemsize for a in args[1:])
    return pl.pallas_call(
        body,
        out_shape=outs,
        in_specs=[pl.BlockSpec(memory_space=pltpu.SMEM)]
        + [pl.BlockSpec(memory_space=pltpu.VMEM)] * (len(args) - 1),
        out_specs=jax.tree.map(lambda _: pl.BlockSpec(memory_space=pltpu.VMEM), outs),
        scratch_shapes=list(scratch),
        compiler_params=pltpu.CompilerParams(vmem_limit_bytes=limit << 20),
        cost_estimate=pl.CostEstimate(flops=flops, bytes_accessed=size, transcendentals=0),
    )(*args)


def shape(*dims, dtype=bf16):
    return jax.ShapeDtypeStruct(dims, dtype)


def spans(t):
    return pl.ds(pl.multiple_of(t * 64, 64), 64)


def halves(t):
    return pl.ds(pl.multiple_of(t * 256, 256), 256)


def pack_body(place, w_ref, o_ref, extra_ref, *outs):
    y = place[0]
    for k, out in enumerate(outs):
        j = lax.rem(y + k, 4)
        columns = pl.ds(pl.multiple_of(j * 256, 256), 256)
        for row, component in enumerate((1, 2, 0)):
            out[row * 64 : row * 64 + 64, :] = w_ref[component, :, columns]
        out[192:256, :] = o_ref[:, columns]
        out[256:264, :] = extra_ref[lax.div(j, 2)]


def sort_body(place, a, b, c, d, key_value, query_out, steps):
    slot = 2 * lax.rem(place[0], 2) + place[2]
    for k, piece in enumerate((a, b, c, d)):
        source = lax.rem(slot + 4 - k, 4)
        rows = pl.ds(pl.multiple_of(source * 64, 64), 64)
        for i in range(2):
            key_value[i, rows, :] = piece[i * 64 : i * 64 + 64, :]
            query_out[i, rows, :] = piece[i * 64 + 128 : i * 64 + 192, :]
        steps[source] = piece[256:264, :].astype(f32)


def project_body(place, rows, *refs):
    blocks, out, stack = refs[:8], refs[8], refs[9]

    def fill(which, carry):
        for m in range(8):
            stack[which, m * 256 : m * 256 + 256, :] = blocks[m][which]
        return carry

    lax.fori_loop(0, 2, fill, 0)

    def part(i, carry):
        out[halves(i), :] = dot(rows[halves(lax.rem(i, 2)), :], stack[lax.div(i, 2)], 1, 0)
        return carry

    lax.fori_loop(0, 4, part, 0)


def query_body(place, rows, *refs):
    blocks, (query_out, out_own, sent, stack) = refs[:8], refs[8:]
    z, core = place[1], place[2]
    for m in range(8):
        stack[m * 256 : m * 256 + 256, :] = blocks[m][0]

    def part(i, carry):
        query_out[halves(i), :] = dot(rows[halves(i), :], stack[...], 1, 0)
        return carry

    lax.fori_loop(0, 2, part, 0)

    def split(t, carry):
        value = query_out[spans(t), :]
        coarse = value.astype(bf16)
        sent[spans(t), :] = coarse
        sent[spans(t + 8), :] = (value - coarse.astype(f32)).astype(bf16)
        return carry

    lax.fori_loop(0, 8, split, 0)
    for m in range(8):
        source = lax.rem(z + m, 8)
        start = lax.rem(source, 4) * 256
        kept = lax.div(source, 4) == core

        @pl.when(kept)
        def _():
            out_own[pl.ds(pl.multiple_of(start, 256), 256), :] = blocks[m][1]

        @pl.when(jnp.logical_not(kept))
        def _():
            sent[pl.ds(pl.multiple_of(start + 1024, 256), 256), :] = blocks[m][1]


def sides(own, other, first):
    return jnp.where(first, own, other), jnp.where(first, other, own)


def normed(own, other, first, epsilon):
    low, high = sides(own, other, first)
    square = jnp.sum(low * low, axis=-1, keepdims=True) + jnp.sum(high * high, axis=-1, keepdims=True)
    factor = lax.rsqrt(square / 512 + epsilon)
    return (low * factor).astype(bf16), (high * factor).astype(bf16)


def grads_body(place, pair_own, pair_other, step, weights, own_out, *refs):
    outs, (left, right, pre, whole) = refs[:7], refs[7:]
    z, core = place[1], place[2]
    first = core == 0
    half = pl.ds(pl.multiple_of(core * 256, 256), 256)

    def inputs(t, carry):
        span, down = spans(t), spans(t + 8)
        low, high = normed(pair_own[span, :], pair_other[span, :], first, 1e-06)
        left[0, span, 0:256] = low
        left[0, span, 256:512] = high
        scale = step[span, :]
        low, high = sides(pair_own[down, :], pair_other[down, :], first)
        left[1, span, 0:256] = (-(scale * low.astype(bf16).astype(f32))).astype(bf16)
        left[1, span, 256:512] = (-(scale * high.astype(bf16).astype(f32))).astype(bf16)
        return carry

    lax.fori_loop(0, 8, inputs, 0)

    def inner(i, carry):
        pre[i] = dot(left[lax.div(i, 2)], weights[i, :, half], 1, 0)
        return carry

    lax.fori_loop(0, 3, inner, 0)

    def middle(t, carry):
        span = spans(t)
        gate, up, back = pre[0, span, :], pre[1, span, :], pre[2, span, :]
        squash = jax.nn.sigmoid(gate)
        right[2, span, :] = (gate * squash * up).astype(bf16)
        right[0, span, :] = (back * up * squash * (1.0 + gate * (1.0 - squash))).astype(bf16)
        right[1, span, :] = (back * gate * squash).astype(bf16)
        return carry

    lax.fori_loop(0, 8, middle, 0)

    def outer(i, carry):
        whole[i] = dot(left[lax.div(i, 2)], right[i], 0, 0)
        for m in range(8):
            value = whole[i, spans(lax.rem(z + m, 8)), :]
            if m == 0:
                own_out[spans(i), :] = value
            else:
                outs[m - 1][spans(i), :] = value.astype(bf16)
        return carry

    lax.fori_loop(0, 3, outer, 0)


def order_body(place, *refs):
    for m in range(8):
        for i in range(3):
            refs[9][spans(i * 8 + lax.rem(place[1] + m, 8)), :] = refs[m][i * 64 : i * 64 + 64, :]

    def tile(t, carry):
        refs[9][spans(t + 24), :] = refs[8][spans(t), :]
        return carry

    lax.fori_loop(0, 32, tile, 0)


def newton_body(place, own, other, weights, rate, out, x_ref):
    first = place[2] == 0

    def start(m, carry):
        def square(t, total):
            low, high = own[spans(m * 8 + t), :].astype(f32), other[spans(m * 8 + t), :].astype(f32)
            return total + low * low + high * high

        total = jnp.sum(lax.fori_loop(0, 8, square, jnp.zeros((64, 256), f32)))
        factor = 1.0 / (jnp.sqrt(jnp.full((1, 1), total)) + 1e-06)

        def scale(t, inner):
            low, high = sides(own[spans(m * 8 + t), :], other[spans(m * 8 + t), :], first)
            x_ref[m, spans(t), 0:256] = (low.astype(f32) * factor).astype(bf16)
            x_ref[m, spans(t), 256:512] = (high.astype(f32) * factor).astype(bf16)
            return inner

        return lax.fori_loop(0, 8, scale, carry)

    lax.fori_loop(0, 3, start, 0)

    def iteration(i, carry):
        m = lax.rem(i, 3)
        x = x_ref[m]
        gram = dot(x, x, 0, 0).astype(bf16)
        cubic = dot(x, gram, 1, 0)
        quintic = dot(cubic.astype(bf16), gram, 1, 0)
        x_ref[m] = (
            coef_linear * x.astype(f32) + coef_cubic * cubic + coef_quintic * quintic
        ).astype(bf16)
        return carry

    lax.fori_loop(0, 3 * NS_ITERS, iteration, 0)

    def update(i, carry):
        m, span = lax.div(i, 8), spans(lax.rem(i, 8))
        change = rate[0, 0] * x_ref[m, span, :].astype(f32)
        out[m, span, :] = (weights[m, span, :].astype(f32) - change).astype(bf16)
        return carry

    lax.fori_loop(0, 24, update, 0)


def apply_body(place, query_own, out_own, other, updated, out, top, bottom, *refs):
    query, pre_ref, hidden, mixed, left_ref, right_ref, full = refs
    first = place[2] == 0

    def inputs(t, carry):
        span = spans(t)
        arrived = other[spans(t + 24), :].astype(f32) + other[spans(t + 32), :].astype(f32)
        low, high = normed(query_own[span, :], arrived, first, 1e-06)
        query[span, 0:256] = low
        query[span, 256:512] = high
        return carry

    lax.fori_loop(0, 8, inputs, 0)

    def inner(i, carry):
        part = halves(lax.rem(i, 2))
        pre_ref[lax.div(i, 2), part, :] = dot(query[part, :], updated[lax.div(i, 2)], 1, 0)
        return carry

    lax.fori_loop(0, 4, inner, 0)

    def middle(t, carry):
        gate = pre_ref[0, spans(t), :]
        hidden[spans(t), :] = (gate * jax.nn.sigmoid(gate) * pre_ref[1, spans(t), :]).astype(bf16)
        return carry

    lax.fori_loop(0, 8, middle, 0)

    def outer(i, carry):
        mixed[halves(i), :] = dot(hidden[halves(i), :], updated[2], 1, 1)
        return carry

    lax.fori_loop(0, 2, outer, 0)

    def scaled(t, carry):
        value = mixed[spans(t), :]
        value = value * lax.rsqrt(jnp.mean(value * value, axis=-1, keepdims=True) + 1e-05)
        left, right = sides(value[:, 0:256], value[:, 256:512], first)
        left_ref[spans(t), :] = left.astype(bf16)
        right_ref[spans(t), :] = right.astype(bf16)
        return carry

    lax.fori_loop(0, 8, scaled, 0)

    def last(i, carry):
        full[i] = dot(left_ref[...], out_own[halves(i), :], 1, 1) + dot(
            right_ref[...], other[halves(i + 10), :], 1, 1
        )
        columns = halves(i)
        out[:, columns] = full[i, 0:384, :]
        top[:, columns] = full[i, 384:448, :].astype(bf16)
        bottom[:, columns] = full[i, 448:512, :].astype(bf16)
        return carry

    lax.fori_loop(0, 4, last, 0)


def relay_body(place, partial, top, bottom, low_out, high_out):
    low_out[0:64, :] = partial[128:192, :].astype(bf16)
    low_out[64:128, :] = (partial[192:256, :] + bottom[...].astype(f32)).astype(bf16)
    high_out[0:64, :] = (partial[256:320, :] + top[...].astype(f32)).astype(bf16)
    high_out[64:128, :] = partial[320:384, :].astype(bf16)


def payload_body(place, weights, momentum, scalars, out):
    def tile(i, carry):
        out[spans(i), :] = weights[lax.rem(place[0], 2), lax.div(i, 8), spans(lax.rem(i, 8)), :]
        return carry

    lax.fori_loop(0, 24, tile, 0)
    out[1536:1728, :] = momentum[...]
    out[1728:1736, :] = scalars[...]


def choose_body(place, mine, arrived, weights_out, momentum_out, scalars_out):
    owner = lax.div(place[0], 2) == place[2]
    columns = pl.ds(pl.multiple_of(place[2] * 256, 256), 256)

    def take(source):
        def tile(i, carry):
            weights_out[lax.div(i, 8), spans(lax.rem(i, 8)), :] = source[spans(i), :]
            return carry

        lax.fori_loop(0, 24, tile, 0)
        momentum_out[...] = source[1536:1728, columns].astype(f32)
        scalars_out[...] = source[1728:1736, :].astype(f32)

    @pl.when(owner)
    def _():
        take(mine)

    @pl.when(jnp.logical_not(owner))
    def _():
        take(arrived)


def copies(moves, sems):
    started = [pltpu.make_async_copy(a, b, sems.at[i]) for i, (a, b) in enumerate(moves)]
    for copy in started:
        copy.start()
    for copy in started:
        copy.wait()


def emit_body(place, made, across, outward, out, sems):
    slot = lax.rem(place[0], 2)
    owner = lax.div(place[0], 2) == place[2]

    @pl.when(owner)
    def _():
        copies([(made, out.at[slot]), (across, out.at[1 - slot])], sems)

    @pl.when(jnp.logical_not(owner))
    def _():
        copies([(outward, out.at[1 - slot])], sems)


def finish_body(place, relayed, traded, _, out, sems):
    slot = lax.rem(place[0], 2)

    @pl.when(lax.div(place[0], 2) != place[2])
    def _():
        moves = [
            (relayed, out.at[slot, :, pl.ds(0, 256)]),
            (traded, out.at[slot, :, pl.ds(256, 256)]),
        ]
        copies(moves, sems)


def turn_body(place, tokens, out):
    for m in range(8):
        start = pl.multiple_of(lax.rem(place[1] + m, 8) * 256, 256)
        out[:, m * 256 : m * 256 + 256] = tokens[:, pl.ds(start, 256)]


def total_body(place, tokens, partial, low, high, out):
    columns = pl.ds(pl.multiple_of(place[2] * 1024, 1024), 1024)

    def tile(t, carry):
        span = pl.ds(pl.multiple_of(t * 16, 16), 16)
        total = tokens[span, columns].astype(f32) + partial[span, :]
        out[span, :] = (total + low[span, :].astype(f32) + high[span, :].astype(f32)).astype(bf16)
        return carry

    lax.fori_loop(0, 8, tile, 0)


def to_head_chips(pieces):
    got = []
    for k, part in enumerate(pieces):
        pairs = []
        for source in range(4):
            for c in range(2):
                j = (source + k) % 4
                pairs.append((source * 2 + c, (2 * c + j // 2) * 2 + j % 2))
        got.append(lax.ppermute(part, ("y", "head"), pairs))
    return got


def ring_gather(chunk, ups, downs):
    up, down = [chunk], [chunk]
    for step in range(4):
        if step < ups:
            up.append(moved(up[-1], "z", 1))
        if step < downs:
            down.append(moved(down[-1], "z", -1))
    return down + up[:0:-1]


def section_step(group_in, w_qkv, w_out, step_sizes, fast_weights, momentum, momentum_decay, fast_rate):
    core, y, z = lax.axis_index("head"), lax.axis_index("y"), lax.axis_index("z")
    place = jnp.stack([y, z, core])

    steps = step_sizes[0].T
    steps_high = lax.reduce_precision(steps, 8, 7)
    extra = jnp.concatenate([steps_high, steps - steps_high], axis=1).astype(bf16)
    extra = jnp.broadcast_to(extra[:, None, :], (2, 8, 256))
    pieces = kernel_call(pack_body, [shape(264, 256)] * 4, [place, w_qkv[0], w_out[0].T, extra])
    key_value, query_out, step_rows = kernel_call(
        sort_body,
        [shape(2, 256, 256), shape(2, 256, 256), shape(4, 8, 256, dtype=f32)],
        [place, *to_head_chips(pieces)],
    )

    key_value_blocks = ring_gather(key_value, 4, 3)
    query_out_blocks = ring_gather(query_out, 3, 4)

    step_all = step_rows[:, 0, :128] + step_rows[:, 0, 128:]
    step = jnp.concatenate(
        [lax.dynamic_index_in_dim(step_all, (y + k) % 4, 0, False) for k in (0, 3, 1, 2)]
    )[:, None]

    tokens, _ = lax.optimization_barrier((group_in[0], pieces[0]))
    turned = kernel_call(turn_body, shape(128, 2048), [place, tokens])
    rows = jnp.concatenate(
        [turned, moved(turned, "y", 1), moved(turned, "y", -1), moved(turned, "y", 2)]
    )

    part = lax.dynamic_slice(momentum[0], (y % 2, 0, z * 64, 0), (1, 3, 64, 512)).reshape(192, 512)
    scalars = jnp.stack([momentum_decay[0], fast_rate[0]])
    scalars = lax.dynamic_index_in_dim(scalars, y % 2, 1, False)
    terms = []
    for _ in range(3):
        term = lax.reduce_precision(scalars, 8, 7)
        terms.append(term)
        scalars = scalars - term
    terms = jnp.pad(jnp.concatenate(terms), (0, 2))
    terms = jnp.broadcast_to(terms[:, None], (8, 512)).astype(bf16)
    part, terms, _ = lax.optimization_barrier((part, terms, pieces[0]))
    mine = kernel_call(payload_body, shape(1736, 512), [place, fast_weights[0], part, terms])
    pairs = [(yy * 2 + yy // 2, yy * 2 + 1 - yy // 2) for yy in range(4)]
    mine_sent = lax.ppermute(mine, ("y", "head"), pairs)
    weights, momentum_own, terms = kernel_call(
        choose_body,
        [shape(3, 512, 512), shape(192, 256, dtype=f32), shape(8, 512, dtype=f32)],
        [place, mine, mine_sent],
    )
    decay = terms[0, 0] + terms[2, 0] + terms[4, 0]
    rate = (terms[1, 0] + terms[3, 0] + terms[5, 0]).reshape(1, 1)

    pair = kernel_call(
        project_body,
        shape(1024, 256, dtype=f32),
        [place, rows, *key_value_blocks],
        flops=2 * 512 * 2048 * 512,
        scratch=[pltpu.VMEM((2, 2048, 256), bf16)],
    )
    pair_other = swapped(pair)
    own_sum, *parts = kernel_call(
        grads_body,
        [shape(192, 256, dtype=f32)] + [shape(192, 256)] * 7,
        [place, pair, pair_other, step, weights],
        flops=2 * 512 * 512 * 256 * 6,
        scratch=[
            pltpu.VMEM((2, 512, 512), bf16),
            pltpu.VMEM((3, 512, 256), bf16),
            pltpu.VMEM((3, 512, 256), f32),
            pltpu.VMEM((3, 512, 256), f32),
        ],
    )
    to_up = moved(parts[3 - 1], "z", 1)
    to_far = moved(parts[4 - 1], "z", 2)
    to_down = moved(parts[5 - 1], "z", -1)
    near = [moved(parts[1 - 1], "z", 1), moved(parts[7 - 1], "z", -1)]
    ahead = (parts[2 - 1].astype(f32) + to_up.astype(f32) + to_far.astype(f32)).astype(bf16)
    behind = (parts[6 - 1].astype(f32) + to_down.astype(f32)).astype(bf16)
    rows, _ = lax.optimization_barrier((rows, parts[3]))
    query_half, out_own, query_sent = kernel_call(
        query_body,
        [shape(512, 256, dtype=f32), shape(1024, 256), shape(2048, 256)],
        [place, rows, *query_out_blocks],
        flops=2 * 512 * 2048 * 256,
        scratch=[pltpu.VMEM((2048, 256), bf16)],
    )
    own_sum, _ = lax.optimization_barrier((own_sum, query_sent))
    total = own_sum
    for term in (*near, moved(ahead, "z", 2), moved(behind, "z", -2)):
        total = total + term.astype(f32)
    moment = (decay * momentum_own + total).astype(bf16)
    around = {0: moment, 2: moved(moment, "z", -2), 6: moved(moment, "z", 2)}
    around[1], around[7] = moved(moment, "z", -1), moved(moment, "z", 1)
    around[3], around[5] = moved(around[2], "z", -1), moved(around[6], "z", 1)
    around[4] = moved(around[2], "z", -2)
    moment_half = kernel_call(
        order_body, shape(3584, 256), [place] + [around[m] for m in range(8)] + [query_sent]
    )

    moment_other = swapped(moment_half)
    made = kernel_call(
        newton_body,
        shape(3, 512, 512),
        [place, moment_half, moment_other, weights, rate],
        flops=2 * 512**3 * 18,
        scratch=[pltpu.VMEM((3, 512, 512), bf16)],
    )

    def along(value, hops):
        return lax.ppermute(value, ("y", "head"), [(a * 2 + c, b * 2 + d) for a, c, b, d in hops])

    outer = [(1, 2), (0, 3), (3, 0), (2, 1)]
    across = along(made, [(a, a // 2, a ^ 1, a // 2) for a in range(4)])
    outward = along(made, [(a, a // 2, b, a // 2) for a, b in outer])

    partial, top, bottom = kernel_call(
        apply_body,
        [shape(384, 1024, dtype=f32), shape(64, 1024), shape(64, 1024)],
        [place, query_half, out_own, moment_other, made],
        flops=2 * 512**3 * 5,
        scratch=[
            pltpu.VMEM((512, 512), bf16),
            pltpu.VMEM((2, 512, 512), f32),
            pltpu.VMEM((512, 512), bf16),
            pltpu.VMEM((512, 512), f32),
            pltpu.VMEM((512, 256), bf16),
            pltpu.VMEM((512, 256), bf16),
            pltpu.VMEM((4, 512, 256), f32),
        ],
    )
    low, high = kernel_call(
        relay_body,
        [shape(128, 1024)] * 2,
        [place, partial, moved(top, "y", 1), moved(bottom, "y", -1)],
    )
    across, outward, _ = lax.optimization_barrier((across, outward, low))
    relayed = along(across[:, :256], [(a, a // 2, b, a // 2) for a, b in outer])
    traded = along(outward[:, 256:], [(a, 1 - a // 2, a ^ 1, 1 - a // 2) for a in range(4)])

    def emit(body, values, **more):
        count = len(values)
        return pl.pallas_call(
            body,
            out_shape=shape(2, 3, 512, 512),
            in_specs=[pl.BlockSpec(memory_space=pltpu.SMEM)]
            + [pl.BlockSpec(memory_space=pltpu.VMEM)] * count
            + [pl.BlockSpec(memory_space=pl.ANY)] * (len(more) > 0),
            out_specs=pl.BlockSpec(memory_space=pl.ANY),
            scratch_shapes=[pltpu.SemaphoreType.DMA((2,))],
            compiler_params=pltpu.CompilerParams(vmem_limit_bytes=16 << 20),
            cost_estimate=pl.CostEstimate(flops=0, bytes_accessed=3 << 20, transcendentals=0),
            **({"input_output_aliases": {count + 1: 0}} if more else {}),
        )(place, *values, *more.values())

    fast_next = emit(emit_body, (made, across, outward))
    fast_next = emit(finish_body, (relayed, traded), base=fast_next)
    sent_low, sent_high = moved(low, "y", -1), moved(high, "y", 1)
    layer_out = kernel_call(
        total_body, shape(128, 1024), [place, group_in[0], partial, sent_low, sent_high]
    )
    handed = moved(layer_out[None], "section", 1)
    return (handed, fast_next[None])


def solution(mesh):
    torus = Mesh(
        mesh.devices.reshape(mesh.shape["section"], 8, 4, mesh.shape["head"]),
        ("section", "z", "y", "head"),
    )
    return jax.shard_map(
        section_step,
        mesh=torus,
        in_specs=(
            P("section", TOK, None),
            P("section", None, TOK, "head"),
            P("section", "head", TOK),
            P("section", TOK, "head"),
            P("section", "head", None, None, None),
            P("section", "head", None, None, None),
            P("section", "head"),
            P("section", "head"),
        ),
        out_specs=(P("section", TOK, "head"), P("section", "head", None, None, None)),
        check_vma=False,
    )
```

```python
import jax
import jax.numpy as jnp
from jax import lax
from jax.experimental import pallas as pl
from jax.experimental.pallas import tpu as pltpu
from jax.sharding import Mesh
from jax.sharding import PartitionSpec as P


NS_ITERS = 2
TOK = ("z", "y")

coef_linear = 3.4445
coef_cubic = -4.775
coef_quintic = 2.0315

bf16 = jnp.bfloat16
f32 = jnp.float32


def moved(value, axis, steps):
    count = lax.axis_size(axis)
    return lax.ppermute(value, axis, [(i, (i + steps) % count) for i in range(count)])


def swapped(value):
    return lax.ppermute(value, "head", [(0, 1), (1, 0)])


def dot(a, b, ca, cb):
    return lax.dot_general(a, b, (((ca,), (cb,)), ((), ())), preferred_element_type=f32)


def kernel_call(body, outs, args, flops=0, scratch=(), limit=24):
    size = sum(a.size * a.dtype.itemsize for a in args[1:])
    return pl.pallas_call(
        body,
        out_shape=outs,
        in_specs=[pl.BlockSpec(memory_space=pltpu.SMEM)]
        + [pl.BlockSpec(memory_space=pltpu.VMEM)] * (len(args) - 1),
        out_specs=jax.tree.map(lambda _: pl.BlockSpec(memory_space=pltpu.VMEM), outs),
        scratch_shapes=list(scratch),
        compiler_params=pltpu.CompilerParams(vmem_limit_bytes=limit << 20),
        cost_estimate=pl.CostEstimate(flops=flops, bytes_accessed=size, transcendentals=0),
    )(*args)


def shape(*dims, dtype=bf16):
    return jax.ShapeDtypeStruct(dims, dtype)


def spans(t):
    return pl.ds(pl.multiple_of(t * 64, 64), 64)


def halves(t):
    return pl.ds(pl.multiple_of(t * 256, 256), 256)


def pack_body(place, steps, w_hbm, o_hbm, *refs):
    outs, (w_ref, o_ref, sems) = refs[:4], refs[4:]
    fetches = [pltpu.make_async_copy(w_hbm, w_ref, sems.at[0]), pltpu.make_async_copy(o_hbm, o_ref, sems.at[1])]
    for fetch in fetches:
        fetch.start()
    for fetch in fetches:
        fetch.wait()
    for k, out in enumerate(outs):
        j = lax.rem(place[0] + k, 4)
        columns = pl.ds(pl.multiple_of(j * 256, 256), 256)
        for row, component in enumerate((1, 2, 0)):
            out[row * 64 : row * 64 + 64, :] = w_ref[component, :, columns]
        out[192:256, :] = o_ref[:, columns]
        step = jnp.broadcast_to(steps[pl.ds(lax.div(j, 2), 1), :], (8, 128))
        coarse = step.astype(bf16)
        out[256:264, 0:128] = coarse
        out[256:264, 128:256] = (step - coarse.astype(f32)).astype(bf16)


def sort_body(place, a, b, c, d, key_value, query_out, steps):
    slot = 2 * lax.rem(place[0], 2) + place[2]
    for k, piece in enumerate((a, b, c, d)):
        source = lax.rem(slot + 4 - k, 4)
        rows = pl.ds(pl.multiple_of(source * 64, 64), 64)
        for i in range(2):
            key_value[i, rows, :] = piece[i * 64 : i * 64 + 64, :]
            query_out[i, rows, :] = piece[i * 64 + 128 : i * 64 + 192, :]
        steps[source] = piece[256:264, :].astype(f32)


def project_body(place, rows, *refs):
    blocks, out, stack = refs[:8], refs[8], refs[9]

    def fill(which, carry):
        for m in range(8):
            stack[which, m * 256 : m * 256 + 256, :] = blocks[m][which]
        return carry

    lax.fori_loop(0, 2, fill, 0)

    def part(i, carry):
        out[halves(i), :] = dot(rows[halves(lax.rem(i, 2)), :], stack[lax.div(i, 2)], 1, 0)
        return carry

    lax.fori_loop(0, 4, part, 0)


def query_body(place, rows, *refs):
    blocks, (query_out, out_own, sent, stack) = refs[:8], refs[8:]
    z, core = place[1], place[2]
    for m in range(8):
        stack[m * 256 : m * 256 + 256, :] = blocks[m][0]

    def part(i, carry):
        query_out[halves(i), :] = dot(rows[halves(i), :], stack[...], 1, 0)
        return carry

    lax.fori_loop(0, 2, part, 0)

    def split(t, carry):
        value = query_out[spans(t), :]
        coarse = value.astype(bf16)
        sent[spans(t), :] = coarse
        sent[spans(t + 8), :] = (value - coarse.astype(f32)).astype(bf16)
        return carry

    lax.fori_loop(0, 8, split, 0)
    for m in range(8):
        source = lax.rem(z + m, 8)
        start = lax.rem(source, 4) * 256
        kept = lax.div(source, 4) == core

        @pl.when(kept)
        def _():
            out_own[pl.ds(pl.multiple_of(start, 256), 256), :] = blocks[m][1]

        @pl.when(jnp.logical_not(kept))
        def _():
            sent[pl.ds(pl.multiple_of(start + 1024, 256), 256), :] = blocks[m][1]


def sides(own, other, first):
    return jnp.where(first, own, other), jnp.where(first, other, own)


def normed(own, other, first, epsilon):
    low, high = sides(own, other, first)
    square = jnp.sum(low * low, axis=-1, keepdims=True) + jnp.sum(high * high, axis=-1, keepdims=True)
    factor = lax.rsqrt(square / 512 + epsilon)
    return (low * factor).astype(bf16), (high * factor).astype(bf16)


def grads_body(place, pair_own, pair_other, step, weights, own_out, *refs):
    outs, (left, right, pre, whole) = refs[:7], refs[7:]
    z, core = place[1], place[2]
    first = core == 0
    half = pl.ds(pl.multiple_of(core * 256, 256), 256)

    def inputs(t, carry):
        span, down = spans(t), spans(t + 8)
        low, high = normed(pair_own[span, :], pair_other[span, :], first, 1e-06)
        left[0, span, 0:256] = low
        left[0, span, 256:512] = high
        scale = step[span, :]
        low, high = sides(pair_own[down, :], pair_other[down, :], first)
        left[1, span, 0:256] = (-(scale * low.astype(bf16).astype(f32))).astype(bf16)
        left[1, span, 256:512] = (-(scale * high.astype(bf16).astype(f32))).astype(bf16)
        return carry

    lax.fori_loop(0, 8, inputs, 0)

    def inner(i, carry):
        pre[i] = dot(left[lax.div(i, 2)], weights[i, :, half], 1, 0)
        return carry

    lax.fori_loop(0, 3, inner, 0)

    def middle(t, carry):
        span = spans(t)
        gate, up, back = pre[0, span, :], pre[1, span, :], pre[2, span, :]
        squash = jax.nn.sigmoid(gate)
        right[2, span, :] = (gate * squash * up).astype(bf16)
        right[0, span, :] = (back * up * squash * (1.0 + gate * (1.0 - squash))).astype(bf16)
        right[1, span, :] = (back * gate * squash).astype(bf16)
        return carry

    lax.fori_loop(0, 8, middle, 0)

    def outer(i, carry):
        whole[i] = dot(left[lax.div(i, 2)], right[i], 0, 0)
        for m in range(8):
            value = whole[i, spans(lax.rem(z + m, 8)), :]
            if m == 0:
                own_out[spans(i), :] = value
            else:
                outs[m - 1][spans(i), :] = value.astype(bf16)
        return carry

    lax.fori_loop(0, 3, outer, 0)


def order_body(place, *refs):
    for m in range(8):
        for i in range(3):
            refs[9][spans(i * 8 + lax.rem(place[1] + m, 8)), :] = refs[m][i * 64 : i * 64 + 64, :]

    def tile(t, carry):
        refs[9][spans(t + 24), :] = refs[8][spans(t), :]
        return carry

    lax.fori_loop(0, 32, tile, 0)


def newton_body(place, own, other, weights, rate, top, bottom, x_ref):
    first = place[2] == 0

    def start(m, carry):
        def square(t, total):
            low, high = own[spans(m * 8 + t), :].astype(f32), other[spans(m * 8 + t), :].astype(f32)
            return total + low * low + high * high

        total = jnp.sum(lax.fori_loop(0, 8, square, jnp.zeros((64, 256), f32)))
        factor = 1.0 / (jnp.sqrt(jnp.full((1, 1), total)) + 1e-06)

        def scale(t, inner):
            low, high = sides(own[spans(m * 8 + t), :], other[spans(m * 8 + t), :], first)
            x_ref[m, spans(t), 0:256] = (low.astype(f32) * factor).astype(bf16)
            x_ref[m, spans(t), 256:512] = (high.astype(f32) * factor).astype(bf16)
            return inner

        return lax.fori_loop(0, 8, scale, carry)

    lax.fori_loop(0, 3, start, 0)

    def iteration(i, carry):
        m = lax.rem(i, 3)
        x = x_ref[m]
        gram = dot(x, x, 1, 1).astype(bf16)
        cubic = dot(gram, x, 1, 0)
        quintic = dot(gram, cubic.astype(bf16), 1, 0)
        x_ref[m] = (
            coef_linear * x.astype(f32) + coef_cubic * cubic + coef_quintic * quintic
        ).astype(bf16)
        return carry

    lax.fori_loop(0, 3 * NS_ITERS, iteration, 0)

    for first_tile, out in ((0, top), (4, bottom)):

        def update(i, carry):
            m, t = lax.div(i, 4), lax.rem(i, 4)
            span = spans(t + first_tile)
            change = rate[0, 0] * x_ref[m, span, :].astype(f32)
            out[m, spans(t), :] = (weights[m, span, :].astype(f32) - change).astype(bf16)
            return carry

        lax.fori_loop(0, 12, update, 0)


def apply_body(place, query_own, out_own, other, upper, lower, out, top, bottom, *refs):
    query, pre_ref, hidden, mixed, left_ref, right_ref, full = refs
    first = place[2] == 0

    def inputs(t, carry):
        span = spans(t)
        arrived = other[spans(t + 24), :].astype(f32) + other[spans(t + 32), :].astype(f32)
        low, high = normed(query_own[span, :], arrived, first, 1e-06)
        query[span, 0:256] = low
        query[span, 256:512] = high
        return carry

    lax.fori_loop(0, 8, inputs, 0)

    def inner(i, carry):
        part = halves(lax.rem(i, 2))
        which = lax.div(i, 2)
        pre_ref[which, part, :] = dot(query[part, 0:256], upper[which], 1, 0) + dot(
            query[part, 256:512], lower[which], 1, 0
        )
        return carry

    lax.fori_loop(0, 4, inner, 0)

    def middle(t, carry):
        gate = pre_ref[0, spans(t), :]
        hidden[spans(t), :] = (gate * jax.nn.sigmoid(gate) * pre_ref[1, spans(t), :]).astype(bf16)
        return carry

    lax.fori_loop(0, 8, middle, 0)

    def outer(i, carry):
        mixed[halves(i), 0:256] = dot(hidden[halves(i), :], upper[2], 1, 1)
        mixed[halves(i), 256:512] = dot(hidden[halves(i), :], lower[2], 1, 1)
        return carry

    lax.fori_loop(0, 2, outer, 0)

    def scaled(t, carry):
        value = mixed[spans(t), :]
        value = value * lax.rsqrt(jnp.mean(value * value, axis=-1, keepdims=True) + 1e-05)
        left, right = sides(value[:, 0:256], value[:, 256:512], first)
        left_ref[spans(t), :] = left.astype(bf16)
        right_ref[spans(t), :] = right.astype(bf16)
        return carry

    lax.fori_loop(0, 8, scaled, 0)

    def last(i, carry):
        full[i] = dot(left_ref[...], out_own[halves(i), :], 1, 1) + dot(
            right_ref[...], other[halves(i + 10), :], 1, 1
        )
        columns = halves(i)
        out[:, columns] = full[i, 0:384, :]
        top[:, columns] = full[i, 384:448, :].astype(bf16)
        bottom[:, columns] = full[i, 448:512, :].astype(bf16)
        return carry

    lax.fori_loop(0, 4, last, 0)


def relay_body(place, partial, top, bottom, low_out, high_out):
    low_out[0:64, :] = partial[128:192, :].astype(bf16)
    low_out[64:128, :] = (partial[192:256, :] + bottom[...].astype(f32)).astype(bf16)
    high_out[0:64, :] = (partial[256:320, :] + top[...].astype(f32)).astype(bf16)
    high_out[64:128, :] = partial[320:384, :].astype(bf16)


def payload_body(place, weights, momentum, scalars, out):
    def tile(i, carry):
        out[spans(i), :] = weights[lax.rem(place[0], 2), lax.div(i, 8), spans(lax.rem(i, 8)), :]
        return carry

    lax.fori_loop(0, 24, tile, 0)
    out[1536:1728, :] = momentum[...]
    out[1728:1736, :] = scalars[...]


def choose_body(place, mine, arrived, weights_out, momentum_out, scalars_out):
    owner = lax.div(place[0], 2) == place[2]
    columns = pl.ds(pl.multiple_of(place[2] * 256, 256), 256)

    def take(source):
        def tile(i, carry):
            weights_out[lax.div(i, 8), spans(lax.rem(i, 8)), :] = source[spans(i), :]
            return carry

        lax.fori_loop(0, 24, tile, 0)
        momentum_out[...] = source[1536:1728, columns].astype(f32)
        scalars_out[...] = source[1728:1736, :].astype(f32)

    @pl.when(owner)
    def _():
        take(mine)

    @pl.when(jnp.logical_not(owner))
    def _():
        take(arrived)


def copies(moves, sems):
    started = [pltpu.make_async_copy(a, b, sems.at[i]) for i, (a, b) in enumerate(moves)]
    for copy in started:
        copy.start()
    for copy in started:
        copy.wait()


def emit_body(place, made_top, made_bottom, across_top, across_bottom, outward_top, outward_bottom, out, sems):
    slot = lax.rem(place[0], 2)
    owner = lax.div(place[0], 2) == place[2]

    def head(top, bottom, which):
        return [(top, out.at[which, :, pl.ds(0, 256)]), (bottom, out.at[which, :, pl.ds(256, 256)])]

    @pl.when(owner)
    def _():
        copies(head(made_top, made_bottom, slot) + head(across_top, across_bottom, 1 - slot), sems)

    @pl.when(jnp.logical_not(owner))
    def _():
        copies(head(outward_top, outward_bottom, 1 - slot), sems)


def finish_body(place, relayed, traded, _, out, sems):
    slot = lax.rem(place[0], 2)

    @pl.when(lax.div(place[0], 2) != place[2])
    def _():
        moves = [
            (relayed, out.at[slot, :, pl.ds(0, 256)]),
            (traded, out.at[slot, :, pl.ds(256, 256)]),
        ]
        copies(moves, sems)


def turn_body(place, tokens, out):
    for m in range(8):
        start = pl.multiple_of(lax.rem(place[1] + m, 8) * 256, 256)
        out[:, m * 256 : m * 256 + 256] = tokens[:, pl.ds(start, 256)]


def join_body(place, *refs):
    def tile(t, carry):
        for i in range(4):
            target = pl.ds(pl.multiple_of(t * 16 + i * 128, 16), 16)
            refs[4][target, :] = refs[i][pl.ds(pl.multiple_of(t * 16, 16), 16), :]
        return carry

    lax.fori_loop(0, 8, tile, 0)


def total_body(place, tokens, partial, low, high, out):
    columns = pl.ds(pl.multiple_of(place[2] * 1024, 1024), 1024)

    def tile(t, carry):
        span = pl.ds(pl.multiple_of(t * 16, 16), 16)
        total = tokens[span, columns].astype(f32) + partial[span, :]
        out[span, :] = (total + low[span, :].astype(f32) + high[span, :].astype(f32)).astype(bf16)
        return carry

    lax.fori_loop(0, 8, tile, 0)


def to_head_chips(pieces):
    got = []
    for k, part in enumerate(pieces):
        pairs = []
        for source in range(4):
            for c in range(2):
                j = (source + k) % 4
                pairs.append((source * 2 + c, (2 * c + j // 2) * 2 + j % 2))
        got.append(lax.ppermute(part, ("y", "head"), pairs))
    return got


def ring_gather(chunk, ups, downs):
    up, down = [chunk], [chunk]
    for step in range(4):
        if step < ups:
            up.append(moved(up[-1], "z", 1))
        if step < downs:
            down.append(moved(down[-1], "z", -1))
    return down + up[:0:-1]


def section_step(group_in, w_qkv, w_out, step_sizes, fast_weights, momentum, momentum_decay, fast_rate):
    core, y, z = lax.axis_index("head"), lax.axis_index("y"), lax.axis_index("z")
    place = jnp.stack([y, z, core])

    pieces = pl.pallas_call(
        pack_body,
        name="pack",
        out_shape=[shape(264, 256)] * 4,
        in_specs=[pl.BlockSpec(memory_space=pltpu.SMEM), pl.BlockSpec(memory_space=pltpu.VMEM)]
        + [pl.BlockSpec(memory_space=pl.ANY)] * 2,
        out_specs=[pl.BlockSpec(memory_space=pltpu.VMEM)] * 4,
        scratch_shapes=[
            pltpu.VMEM((3, 64, 1024), bf16),
            pltpu.VMEM((64, 1024), bf16),
            pltpu.SemaphoreType.DMA((2,)),
        ],
        compiler_params=pltpu.CompilerParams(vmem_limit_bytes=16 << 20),
        cost_estimate=pl.CostEstimate(flops=0, bytes_accessed=1 << 20, transcendentals=0),
    )(place, step_sizes[0].T, w_qkv[0], w_out[0].T)
    key_value, query_out, step_rows = kernel_call(
        sort_body,
        [shape(2, 256, 256), shape(2, 256, 256), shape(4, 8, 256, dtype=f32)],
        [place, *to_head_chips(pieces)],
    )

    key_value_blocks = ring_gather(key_value, 4, 3)
    query_out_blocks = ring_gather(query_out, 3, 4)

    step_all = step_rows[:, 0, :128] + step_rows[:, 0, 128:]
    step = jnp.concatenate(
        [lax.dynamic_index_in_dim(step_all, (y + k) % 4, 0, False) for k in (0, 3, 1, 2)]
    )[:, None]

    tokens, _ = lax.optimization_barrier((group_in[0], pieces[0]))
    turned = kernel_call(turn_body, shape(128, 2048), [place, tokens])
    rows = kernel_call(
        join_body,
        shape(512, 2048),
        [place, turned] + [moved(turned, "y", hop) for hop in (1, -1, 2)],
    )

    part = lax.dynamic_slice(momentum[0], (y % 2, 0, z * 64, 0), (1, 3, 64, 512)).reshape(192, 512)
    scalars = jnp.stack([momentum_decay[0], fast_rate[0]])
    scalars = lax.dynamic_index_in_dim(scalars, y % 2, 1, False)
    terms = []
    for _ in range(3):
        term = lax.reduce_precision(scalars, 8, 7)
        terms.append(term)
        scalars = scalars - term
    terms = jnp.pad(jnp.concatenate(terms), (0, 2))
    terms = jnp.broadcast_to(terms[:, None], (8, 512)).astype(bf16)
    part, terms, _ = lax.optimization_barrier((part, terms, pieces[0]))
    mine = kernel_call(payload_body, shape(1736, 512), [place, fast_weights[0], part, terms])
    pairs = [(yy * 2 + yy // 2, yy * 2 + 1 - yy // 2) for yy in range(4)]
    mine_sent = lax.ppermute(mine, ("y", "head"), pairs)
    weights, momentum_own, terms = kernel_call(
        choose_body,
        [shape(3, 512, 512), shape(192, 256, dtype=f32), shape(8, 512, dtype=f32)],
        [place, mine, mine_sent],
    )
    decay = terms[0, 0] + terms[2, 0] + terms[4, 0]
    rate = (terms[1, 0] + terms[3, 0] + terms[5, 0]).reshape(1, 1)

    pair = kernel_call(
        project_body,
        shape(1024, 256, dtype=f32),
        [place, rows, *key_value_blocks],
        flops=2 * 512 * 2048 * 512,
        scratch=[pltpu.VMEM((2, 2048, 256), bf16)],
    )
    pair_other = swapped(pair)
    own_sum, *parts = kernel_call(
        grads_body,
        [shape(192, 256, dtype=f32)] + [shape(192, 256)] * 7,
        [place, pair, pair_other, step, weights],
        flops=2 * 512 * 512 * 256 * 6,
        scratch=[
            pltpu.VMEM((2, 512, 512), bf16),
            pltpu.VMEM((3, 512, 256), bf16),
            pltpu.VMEM((3, 512, 256), f32),
            pltpu.VMEM((3, 512, 256), f32),
        ],
    )
    to_up = moved(parts[3 - 1], "z", 1)
    to_far = moved(parts[4 - 1], "z", 2)
    to_down = moved(parts[5 - 1], "z", -1)
    near = [moved(parts[1 - 1], "z", 1), moved(parts[7 - 1], "z", -1)]
    ahead = (parts[2 - 1].astype(f32) + to_up.astype(f32) + to_far.astype(f32)).astype(bf16)
    behind = (parts[6 - 1].astype(f32) + to_down.astype(f32)).astype(bf16)
    rows, _ = lax.optimization_barrier((rows, parts[3]))
    query_half, out_own, query_sent = kernel_call(
        query_body,
        [shape(512, 256, dtype=f32), shape(1024, 256), shape(2048, 256)],
        [place, rows, *query_out_blocks],
        flops=2 * 512 * 2048 * 256,
        scratch=[pltpu.VMEM((2048, 256), bf16)],
    )
    own_sum, _ = lax.optimization_barrier((own_sum, query_sent))
    total = own_sum
    for term in (*near, moved(ahead, "z", 2), moved(behind, "z", -2)):
        total = total + term.astype(f32)
    moment = (decay * momentum_own + total).astype(bf16)
    around = {0: moment, 2: moved(moment, "z", -2), 6: moved(moment, "z", 2)}
    around[1], around[7] = moved(moment, "z", -1), moved(moment, "z", 1)
    around[3], around[5] = moved(around[2], "z", -1), moved(around[6], "z", 1)
    around[4] = moved(around[2], "z", -2)
    moment_half = kernel_call(
        order_body, shape(3584, 256), [place] + [around[m] for m in range(8)] + [query_sent]
    )

    moment_other = swapped(moment_half)
    made_top, made_bottom = kernel_call(
        newton_body,
        [shape(3, 256, 512)] * 2,
        [place, moment_half, moment_other, weights, rate],
        flops=2 * 512**3 * 18,
        scratch=[pltpu.VMEM((3, 512, 512), bf16)],
    )

    def along(value, hops):
        return lax.ppermute(value, ("y", "head"), [(a * 2 + c, b * 2 + d) for a, c, b, d in hops])

    outer = [(1, 2), (0, 3), (3, 0), (2, 1)]

    def first_hop(value):
        across = along(value, [(a, a // 2, a ^ 1, a // 2) for a in range(4)])
        return across, along(value, [(a, a // 2, b, a // 2) for a, b in outer])

    across_top, outward_top = first_hop(made_top)
    across_bottom, outward_bottom = first_hop(made_bottom)

    partial, top, bottom = kernel_call(
        apply_body,
        [shape(384, 1024, dtype=f32), shape(64, 1024), shape(64, 1024)],
        [place, query_half, out_own, moment_other, made_top, made_bottom],
        flops=2 * 512**3 * 5,
        scratch=[
            pltpu.VMEM((512, 512), bf16),
            pltpu.VMEM((2, 512, 512), f32),
            pltpu.VMEM((512, 512), bf16),
            pltpu.VMEM((512, 512), f32),
            pltpu.VMEM((512, 256), bf16),
            pltpu.VMEM((512, 256), bf16),
            pltpu.VMEM((4, 512, 256), f32),
        ],
    )
    low, high = kernel_call(
        relay_body,
        [shape(128, 1024)] * 2,
        [place, partial, moved(top, "y", 1), moved(bottom, "y", -1)],
    )
    relayed = along(across_top, [(a, a // 2, b, a // 2) for a, b in outer])
    traded = along(outward_bottom, [(a, 1 - a // 2, a ^ 1, 1 - a // 2) for a in range(4)])

    def emit(body, values, **more):
        count = len(values)
        return pl.pallas_call(
            body,
            out_shape=shape(2, 3, 512, 512),
            in_specs=[pl.BlockSpec(memory_space=pltpu.SMEM)]
            + [pl.BlockSpec(memory_space=pltpu.VMEM)] * count
            + [pl.BlockSpec(memory_space=pl.ANY)] * (len(more) > 0),
            out_specs=pl.BlockSpec(memory_space=pl.ANY),
            scratch_shapes=[pltpu.SemaphoreType.DMA((4,))],
            compiler_params=pltpu.CompilerParams(vmem_limit_bytes=16 << 20),
            cost_estimate=pl.CostEstimate(flops=0, bytes_accessed=3 << 20, transcendentals=0),
            **({"input_output_aliases": {count + 1: 0}} if more else {}),
        )(place, *values, *more.values())

    fast_next = emit(
        emit_body, (made_top, made_bottom, across_top, across_bottom, outward_top, outward_bottom)
    )
    fast_next = emit(finish_body, (relayed, traded), base=fast_next)
    sent_low, sent_high = moved(low, "y", -1), moved(high, "y", 1)
    layer_out = kernel_call(
        total_body, shape(128, 1024), [place, group_in[0], partial, sent_low, sent_high]
    )
    handed = moved(layer_out[None], "section", 1)
    return (handed, fast_next[None])


def solution(mesh):
    torus = Mesh(
        mesh.devices.reshape(mesh.shape["section"], 8, 4, mesh.shape["head"]),
        ("section", "z", "y", "head"),
    )
    return jax.shard_map(
        section_step,
        mesh=torus,
        in_specs=(
            P("section", TOK, None),
            P("section", None, TOK, "head"),
            P("section", "head", TOK),
            P("section", TOK, "head"),
            P("section", "head", None, None, None),
            P("section", "head", None, None, None),
            P("section", "head"),
            P("section", "head"),
        ),
        out_specs=(P("section", TOK, "head"), P("section", "head", None, None, None)),
        check_vma=False,
    )
```

```python
import jax
import jax.numpy as jnp
from jax import lax
from jax.experimental import pallas as pl
from jax.experimental.pallas import tpu as pltpu
from jax.sharding import Mesh
from jax.sharding import PartitionSpec as P


NS_ITERS = 2
TOK = ("z", "y")

coef_linear = 3.4445
coef_cubic = -4.775
coef_quintic = 2.0315

bf16 = jnp.bfloat16
f32 = jnp.float32


def moved(value, axis, steps):
    count = lax.axis_size(axis)
    return lax.ppermute(value, axis, [(i, (i + steps) % count) for i in range(count)])


def swapped(value):
    return lax.ppermute(value, "head", [(0, 1), (1, 0)])


def dot(a, b, ca, cb):
    return lax.dot_general(a, b, (((ca,), (cb,)), ((), ())), preferred_element_type=f32)


def kernel_call(body, outs, args, flops=0, scratch=(), limit=24):
    size = sum(a.size * a.dtype.itemsize for a in args[1:])
    return pl.pallas_call(
        body,
        out_shape=outs,
        in_specs=[pl.BlockSpec(memory_space=pltpu.SMEM)]
        + [pl.BlockSpec(memory_space=pltpu.VMEM)] * (len(args) - 1),
        out_specs=jax.tree.map(lambda _: pl.BlockSpec(memory_space=pltpu.VMEM), outs),
        scratch_shapes=list(scratch),
        compiler_params=pltpu.CompilerParams(vmem_limit_bytes=limit << 20),
        cost_estimate=pl.CostEstimate(flops=flops, bytes_accessed=size, transcendentals=0),
    )(*args)


def shape(*dims, dtype=bf16):
    return jax.ShapeDtypeStruct(dims, dtype)


def spans(t):
    return pl.ds(pl.multiple_of(t * 64, 64), 64)


def halves(t):
    return pl.ds(pl.multiple_of(t * 256, 256), 256)


def pack_body(place, steps, w_hbm, o_hbm, *refs):
    outs, (w_ref, o_ref, sems) = refs[:4], refs[4:]
    fetches = [pltpu.make_async_copy(w_hbm, w_ref, sems.at[0]), pltpu.make_async_copy(o_hbm, o_ref, sems.at[1])]
    for fetch in fetches:
        fetch.start()
    for fetch in fetches:
        fetch.wait()
    for k, out in enumerate(outs):
        j = lax.rem(place[0] + k, 4)
        columns = pl.ds(pl.multiple_of(j * 256, 256), 256)
        for row, component in enumerate((1, 2, 0)):
            out[row * 64 : row * 64 + 64, :] = w_ref[component, :, columns]
        out[192:256, :] = o_ref[:, columns]
        step = jnp.broadcast_to(steps[pl.ds(lax.div(j, 2), 1), :], (8, 128))
        coarse = step.astype(bf16)
        out[256:264, 0:128] = coarse
        out[256:264, 128:256] = (step - coarse.astype(f32)).astype(bf16)


def sort_body(place, a, b, c, d, key_value, query_out, step):
    slot = 2 * lax.rem(place[0], 2) + place[2]
    for k, piece in enumerate((a, b, c, d)):
        source = lax.rem(slot + 4 - k, 4)
        rows = pl.ds(pl.multiple_of(source * 64, 64), 64)
        for i in range(2):
            key_value[i, rows, :] = piece[i * 64 : i * 64 + 64, :]
            query_out[i, rows, :] = piece[i * 64 + 128 : i * 64 + 192, :]
        terms = piece[256:264, :].astype(f32)
        column = jnp.broadcast_to(terms[0:1, 0:128] + terms[0:1, 128:256], (128, 128)).T
        block = lax.rem(source + 4 - place[0], 4)
        step[pl.ds(pl.multiple_of(block * 128, 128), 128), :] = column


def project_body(place, rows, *refs):
    blocks, out, stack = refs[:8], refs[8], refs[9]

    def fill(which, carry):
        for m in range(8):
            stack[which, m * 256 : m * 256 + 256, :] = blocks[m][which]
        return carry

    lax.fori_loop(0, 2, fill, 0)

    def part(i, carry):
        out[halves(i), :] = dot(rows[halves(lax.rem(i, 2)), :], stack[lax.div(i, 2)], 1, 0)
        return carry

    lax.fori_loop(0, 4, part, 0)


def query_body(place, rows, *refs):
    blocks, (query_out, out_own, sent, stack) = refs[:8], refs[8:]
    z, core = place[1], place[2]
    for m in range(8):
        stack[m * 256 : m * 256 + 256, :] = blocks[m][0]

    def part(i, carry):
        query_out[halves(i), :] = dot(rows[halves(i), :], stack[...], 1, 0)
        return carry

    lax.fori_loop(0, 2, part, 0)

    def split(t, carry):
        value = query_out[spans(t), :]
        coarse = value.astype(bf16)
        sent[spans(t), :] = coarse
        sent[spans(t + 8), :] = (value - coarse.astype(f32)).astype(bf16)
        return carry

    lax.fori_loop(0, 8, split, 0)
    for m in range(8):
        source = lax.rem(z + m, 8)
        start = lax.rem(source, 4) * 256
        kept = lax.div(source, 4) == core

        @pl.when(kept)
        def _():
            out_own[pl.ds(pl.multiple_of(start, 256), 256), :] = blocks[m][1]

        @pl.when(jnp.logical_not(kept))
        def _():
            sent[pl.ds(pl.multiple_of(start + 1024, 256), 256), :] = blocks[m][1]


def sides(own, other, first):
    return jnp.where(first, own, other), jnp.where(first, other, own)


def normed(own, other, first, epsilon):
    low, high = sides(own, other, first)
    square = jnp.sum(low * low, axis=-1, keepdims=True) + jnp.sum(high * high, axis=-1, keepdims=True)
    factor = lax.rsqrt(square / 512 + epsilon)
    return (low * factor).astype(bf16), (high * factor).astype(bf16)


def grads_body(place, pair_own, pair_other, step, weights, own_out, *refs):
    outs, (left, right, pre, whole) = refs[:7], refs[7:]
    z, core = place[1], place[2]
    first = core == 0
    half = pl.ds(pl.multiple_of(core * 256, 256), 256)

    def inputs(t, carry):
        span, down = spans(t), spans(t + 8)
        low, high = normed(pair_own[span, :], pair_other[span, :], first, 1e-06)
        left[0, span, 0:256] = low
        left[0, span, 256:512] = high
        scale = step[span, 0:1]
        low, high = sides(pair_own[down, :], pair_other[down, :], first)
        left[1, span, 0:256] = (-(scale * low.astype(bf16).astype(f32))).astype(bf16)
        left[1, span, 256:512] = (-(scale * high.astype(bf16).astype(f32))).astype(bf16)
        return carry

    lax.fori_loop(0, 8, inputs, 0)

    def inner(i, carry):
        pre[i] = dot(left[lax.div(i, 2)], weights[i, :, half], 1, 0)
        return carry

    lax.fori_loop(0, 3, inner, 0)

    def middle(t, carry):
        span = spans(t)
        gate, up, back = pre[0, span, :], pre[1, span, :], pre[2, span, :]
        squash = jax.nn.sigmoid(gate)
        right[2, span, :] = (gate * squash * up).astype(bf16)
        right[0, span, :] = (back * up * squash * (1.0 + gate * (1.0 - squash))).astype(bf16)
        right[1, span, :] = (back * gate * squash).astype(bf16)
        return carry

    lax.fori_loop(0, 8, middle, 0)

    def outer(i, carry):
        whole[i] = dot(left[lax.div(i, 2)], right[i], 0, 0)
        for m in range(8):
            value = whole[i, spans(lax.rem(z + m, 8)), :]
            if m == 0:
                own_out[spans(i), :] = value
            else:
                outs[m - 1][spans(i), :] = value.astype(bf16)
        return carry

    lax.fori_loop(0, 3, outer, 0)


def order_body(place, *refs):
    for m in range(8):
        for i in range(3):
            refs[9][spans(i * 8 + lax.rem(place[1] + m, 8)), :] = refs[m][i * 64 : i * 64 + 64, :]

    def tile(t, carry):
        refs[9][spans(t + 24), :] = refs[8][spans(t), :]
        return carry

    lax.fori_loop(0, 32, tile, 0)


def newton_body(place, own, other, weights, terms, top, bottom, x_ref):
    first = place[2] == 0

    def start(m, carry):
        def square(t, total):
            low, high = own[spans(m * 8 + t), :].astype(f32), other[spans(m * 8 + t), :].astype(f32)
            return total + low * low + high * high

        total = jnp.sum(lax.fori_loop(0, 8, square, jnp.zeros((64, 256), f32)))
        factor = 1.0 / (jnp.sqrt(jnp.full((1, 1), total)) + 1e-06)

        def scale(t, inner):
            low, high = sides(own[spans(m * 8 + t), :], other[spans(m * 8 + t), :], first)
            x_ref[m, spans(t), 0:256] = (low.astype(f32) * factor).astype(bf16)
            x_ref[m, spans(t), 256:512] = (high.astype(f32) * factor).astype(bf16)
            return inner

        return lax.fori_loop(0, 8, scale, carry)

    lax.fori_loop(0, 3, start, 0)

    def iteration(i, carry):
        m = lax.rem(i, 3)
        x = x_ref[m]
        gram = dot(x, x, 1, 1).astype(bf16)
        cubic = dot(gram, x, 1, 0)
        quintic = dot(gram, cubic.astype(bf16), 1, 0)
        x_ref[m] = (
            coef_linear * x.astype(f32) + coef_cubic * cubic + coef_quintic * quintic
        ).astype(bf16)
        return carry

    lax.fori_loop(0, 3 * NS_ITERS, iteration, 0)

    rate = terms[1:2, 0:1] + terms[3:4, 0:1] + terms[5:6, 0:1]
    for first_tile, out in ((0, top), (4, bottom)):

        def update(i, carry):
            m, t = lax.div(i, 4), lax.rem(i, 4)
            span = spans(t + first_tile)
            change = rate * x_ref[m, span, :].astype(f32)
            out[m, spans(t), :] = (weights[m, span, :].astype(f32) - change).astype(bf16)
            return carry

        lax.fori_loop(0, 12, update, 0)


def apply_body(place, query_own, out_own, other, upper, lower, out, top, bottom, *refs):
    query, pre_ref, hidden, mixed, left_ref, right_ref, full = refs
    first = place[2] == 0

    def inputs(t, carry):
        span = spans(t)
        arrived = other[spans(t + 24), :].astype(f32) + other[spans(t + 32), :].astype(f32)
        low, high = normed(query_own[span, :], arrived, first, 1e-06)
        query[span, 0:256] = low
        query[span, 256:512] = high
        return carry

    lax.fori_loop(0, 8, inputs, 0)

    def inner(i, carry):
        part = halves(lax.rem(i, 2))
        which = lax.div(i, 2)
        pre_ref[which, part, :] = dot(query[part, 0:256], upper[which], 1, 0) + dot(
            query[part, 256:512], lower[which], 1, 0
        )
        return carry

    lax.fori_loop(0, 4, inner, 0)

    def middle(t, carry):
        gate = pre_ref[0, spans(t), :]
        hidden[spans(t), :] = (gate * jax.nn.sigmoid(gate) * pre_ref[1, spans(t), :]).astype(bf16)
        return carry

    lax.fori_loop(0, 8, middle, 0)

    def outer(i, carry):
        mixed[halves(i), 0:256] = dot(hidden[halves(i), :], upper[2], 1, 1)
        mixed[halves(i), 256:512] = dot(hidden[halves(i), :], lower[2], 1, 1)
        return carry

    lax.fori_loop(0, 2, outer, 0)

    def scaled(t, carry):
        value = mixed[spans(t), :]
        value = value * lax.rsqrt(jnp.mean(value * value, axis=-1, keepdims=True) + 1e-05)
        left, right = sides(value[:, 0:256], value[:, 256:512], first)
        left_ref[spans(t), :] = left.astype(bf16)
        right_ref[spans(t), :] = right.astype(bf16)
        return carry

    lax.fori_loop(0, 8, scaled, 0)

    def last(i, carry):
        full[i] = dot(left_ref[...], out_own[halves(i), :], 1, 1) + dot(
            right_ref[...], other[halves(i + 10), :], 1, 1
        )
        columns = halves(i)
        out[0:256, columns] = full[i, 0:256, :]
        out[256:384, columns] = full[i, 384:512, :]
        top[:, columns] = full[i, 256:320, :].astype(bf16)
        bottom[:, columns] = full[i, 320:384, :].astype(bf16)
        return carry

    lax.fori_loop(0, 4, last, 0)


def relay_body(place, partial, top, bottom, low_out, high_out):
    high_out[0:64, :] = (partial[128:192, :] + top[...].astype(f32)).astype(bf16)
    high_out[64:128, :] = partial[192:256, :].astype(bf16)
    low_out[0:64, :] = partial[256:320, :].astype(bf16)
    low_out[64:128, :] = (partial[320:384, :] + bottom[...].astype(f32)).astype(bf16)


def payload_body(place, decays, rates, weights, momentum, out, part, sems):
    slot = lax.rem(place[0], 2)
    rows = pl.ds(pl.multiple_of(place[1] * 64, 64), 64)
    fetches = [pltpu.make_async_copy(momentum.at[slot, :, rows], part, sems.at[3])]
    for m in range(3):
        target = out.at[pl.ds(m * 512, 512)]
        fetches.append(pltpu.make_async_copy(weights.at[slot, m], target, sems.at[m]))
    for fetch in fetches:
        fetch.start()
    terms = jnp.zeros((8, 512), f32)
    which = lax.broadcasted_iota(jnp.int32, (8, 512), 0)
    for i, scalars in enumerate((decays, rates)):
        value = jnp.full((8, 512), scalars[slot])
        for k in range(3):
            term = value.astype(bf16).astype(f32)
            terms = jnp.where(which == 2 * k + i, term, terms)
            value = value - term
    out[1728:1736, :] = terms.astype(bf16)
    for fetch in fetches:
        fetch.wait()
    for m in range(3):
        out[1536 + m * 64 : 1600 + m * 64, :] = part[m]


def sum_body(place, *refs):
    total = refs[0][...].astype(f32)
    for ref in refs[1:-1]:
        total = total + ref[...].astype(f32)
    refs[-1][...] = total.astype(bf16)


def moment_body(place, own, momentum, terms, a, b, c, d, out):
    decay = terms[0:1, 0:1] + terms[2:3, 0:1] + terms[4:5, 0:1]
    total = own[...] + a[...].astype(f32) + b[...].astype(f32) + c[...].astype(f32) + d[...].astype(f32)
    out[...] = (decay * momentum[...] + total).astype(bf16)


def choose_body(place, mine, arrived, weights_out, momentum_out, scalars_out):
    owner = lax.div(place[0], 2) == place[2]
    columns = pl.ds(pl.multiple_of(place[2] * 256, 256), 256)

    def take(source):
        def tile(i, carry):
            weights_out[lax.div(i, 8), spans(lax.rem(i, 8)), :] = source[spans(i), :]
            return carry

        lax.fori_loop(0, 24, tile, 0)
        momentum_out[...] = source[1536:1728, columns].astype(f32)
        scalars_out[...] = source[1728:1736, :].astype(f32)

    @pl.when(owner)
    def _():
        take(mine)

    @pl.when(jnp.logical_not(owner))
    def _():
        take(arrived)


def copies(moves, sems):
    started = [pltpu.make_async_copy(a, b, sems.at[i]) for i, (a, b) in enumerate(moves)]
    for copy in started:
        copy.start()
    for copy in started:
        copy.wait()


def emit_body(place, made_top, made_bottom, across_top, across_bottom, outward_top, outward_bottom, out, sems):
    slot = lax.rem(place[0], 2)
    owner = lax.div(place[0], 2) == place[2]

    def head(top, bottom, which):
        return [(top, out.at[which, :, pl.ds(0, 256)]), (bottom, out.at[which, :, pl.ds(256, 256)])]

    @pl.when(owner)
    def _():
        copies(head(made_top, made_bottom, slot) + head(across_top, across_bottom, 1 - slot), sems)

    @pl.when(jnp.logical_not(owner))
    def _():
        copies(head(outward_top, outward_bottom, 1 - slot), sems)


def finish_body(place, relayed, traded, _, out, sems):
    slot = lax.rem(place[0], 2)

    @pl.when(lax.div(place[0], 2) != place[2])
    def _():
        moves = [
            (relayed, out.at[slot, :, pl.ds(0, 256)]),
            (traded, out.at[slot, :, pl.ds(256, 256)]),
        ]
        copies(moves, sems)


def turn_body(place, tokens, out):
    for m in range(8):
        start = pl.multiple_of(lax.rem(place[1] + m, 8) * 256, 256)
        out[:, m * 256 : m * 256 + 256] = tokens[:, pl.ds(start, 256)]


def join_body(place, *refs):
    def tile(t, carry):
        for i in range(4):
            target = pl.ds(pl.multiple_of(t * 16 + i * 128, 16), 16)
            refs[4][target, :] = refs[i][pl.ds(pl.multiple_of(t * 16, 16), 16), :]
        return carry

    lax.fori_loop(0, 8, tile, 0)


def total_body(place, tokens, partial, low, high, out):
    columns = pl.ds(pl.multiple_of(place[2] * 1024, 1024), 1024)

    def tile(t, carry):
        span = pl.ds(pl.multiple_of(t * 16, 16), 16)
        total = tokens[span, columns].astype(f32) + partial[span, :]
        out[span, :] = (total + low[span, :].astype(f32) + high[span, :].astype(f32)).astype(bf16)
        return carry

    lax.fori_loop(0, 8, tile, 0)


def to_head_chips(pieces):
    got = []
    for k, part in enumerate(pieces):
        pairs = []
        for source in range(4):
            for c in range(2):
                j = (source + k) % 4
                pairs.append((source * 2 + c, (2 * c + j // 2) * 2 + j % 2))
        got.append(lax.ppermute(part, ("y", "head"), pairs))
    return got


def ring_gather(chunk, ups, downs):
    up, down = [chunk], [chunk]
    for step in range(4):
        if step < ups:
            up.append(moved(up[-1], "z", 1))
        if step < downs:
            down.append(moved(down[-1], "z", -1))
    return down + up[:0:-1]


def section_step(group_in, w_qkv, w_out, step_sizes, fast_weights, momentum, momentum_decay, fast_rate):
    core, y, z = lax.axis_index("head"), lax.axis_index("y"), lax.axis_index("z")
    place = jnp.stack([y, z, core])

    pieces = pl.pallas_call(
        pack_body,
        name="pack",
        out_shape=[shape(264, 256)] * 4,
        in_specs=[pl.BlockSpec(memory_space=pltpu.SMEM), pl.BlockSpec(memory_space=pltpu.VMEM)]
        + [pl.BlockSpec(memory_space=pltpu.HBM)] * 2,
        out_specs=[pl.BlockSpec(memory_space=pltpu.VMEM)] * 4,
        scratch_shapes=[
            pltpu.VMEM((3, 64, 1024), bf16),
            pltpu.VMEM((64, 1024), bf16),
            pltpu.SemaphoreType.DMA((2,)),
        ],
        compiler_params=pltpu.CompilerParams(vmem_limit_bytes=16 << 20),
        cost_estimate=pl.CostEstimate(flops=0, bytes_accessed=1 << 20, transcendentals=0),
    )(place, step_sizes[0].T, w_qkv[0], w_out[0].T)
    key_value, query_out, step = kernel_call(
        sort_body,
        [shape(2, 256, 256), shape(2, 256, 256), shape(512, 128, dtype=f32)],
        [place, *to_head_chips(pieces)],
    )

    key_value_blocks = ring_gather(key_value, 4, 3)
    query_out_blocks = ring_gather(query_out, 3, 4)

    tokens, _ = lax.optimization_barrier((group_in[0], pieces[0]))
    turned = kernel_call(turn_body, shape(128, 2048), [place, tokens])
    rows = kernel_call(
        join_body,
        shape(512, 2048),
        [place, turned] + [moved(turned, "y", hop) for hop in (-1, 2, 1)],
    )

    gate, _ = lax.optimization_barrier((momentum_decay[0], pieces[0]))
    mine = pl.pallas_call(
        payload_body,
        name="payload",
        out_shape=shape(1736, 512),
        in_specs=[pl.BlockSpec(memory_space=pltpu.SMEM)] * 3 + [pl.BlockSpec(memory_space=pltpu.HBM)] * 2,
        out_specs=pl.BlockSpec(memory_space=pltpu.VMEM),
        scratch_shapes=[pltpu.VMEM((3, 64, 512), bf16), pltpu.SemaphoreType.DMA((4,))],
        compiler_params=pltpu.CompilerParams(vmem_limit_bytes=16 << 20),
        cost_estimate=pl.CostEstimate(flops=0, bytes_accessed=4 << 20, transcendentals=0),
    )(place, gate, fast_rate[0], fast_weights[0], momentum[0])
    pairs = [(yy * 2 + yy // 2, yy * 2 + 1 - yy // 2) for yy in range(4)]
    mine_sent = lax.ppermute(mine, ("y", "head"), pairs)
    weights, momentum_own, terms = kernel_call(
        choose_body,
        [shape(3, 512, 512), shape(192, 256, dtype=f32), shape(8, 512, dtype=f32)],
        [place, mine, mine_sent],
    )

    pair = kernel_call(
        project_body,
        shape(1024, 256, dtype=f32),
        [place, rows, *key_value_blocks],
        flops=2 * 512 * 2048 * 512,
        scratch=[pltpu.VMEM((2, 2048, 256), bf16)],
    )
    pair_other = swapped(pair)
    own_sum, *parts = kernel_call(
        grads_body,
        [shape(192, 256, dtype=f32)] + [shape(192, 256)] * 7,
        [place, pair, pair_other, step, weights],
        flops=2 * 512 * 512 * 256 * 6,
        scratch=[
            pltpu.VMEM((2, 512, 512), bf16),
            pltpu.VMEM((3, 512, 256), bf16),
            pltpu.VMEM((3, 512, 256), f32),
            pltpu.VMEM((3, 512, 256), f32),
        ],
    )
    to_up = moved(parts[3 - 1], "z", 1)
    to_far = moved(parts[4 - 1], "z", 2)
    to_down = moved(parts[5 - 1], "z", -1)
    near = [moved(parts[1 - 1], "z", 1), moved(parts[7 - 1], "z", -1)]
    block = shape(192, 256)
    ahead = kernel_call(sum_body, block, [place, parts[2 - 1], to_up, to_far])
    behind = kernel_call(sum_body, block, [place, parts[6 - 1], to_down])
    rows, _ = lax.optimization_barrier((rows, parts[3]))
    query_half, out_own, query_sent = kernel_call(
        query_body,
        [shape(512, 256, dtype=f32), shape(1024, 256), shape(2048, 256)],
        [place, rows, *query_out_blocks],
        flops=2 * 512 * 2048 * 256,
        scratch=[pltpu.VMEM((2048, 256), bf16)],
    )
    own_sum, _ = lax.optimization_barrier((own_sum, query_sent))
    sums = [*near, moved(ahead, "z", 2), moved(behind, "z", -2)]
    moment = kernel_call(moment_body, block, [place, own_sum, momentum_own, terms, *sums])
    around = {0: moment, 2: moved(moment, "z", -2), 6: moved(moment, "z", 2)}
    around[1], around[7] = moved(moment, "z", -1), moved(moment, "z", 1)
    around[3], around[5] = moved(around[2], "z", -1), moved(around[6], "z", 1)
    around[4] = moved(around[2], "z", -2)
    moment_half = kernel_call(
        order_body, shape(3584, 256), [place] + [around[m] for m in range(8)] + [query_sent]
    )

    moment_other = swapped(moment_half)
    made_top, made_bottom = kernel_call(
        newton_body,
        [shape(3, 256, 512)] * 2,
        [place, moment_half, moment_other, weights, terms],
        flops=2 * 512**3 * 18,
        scratch=[pltpu.VMEM((3, 512, 512), bf16)],
    )

    def along(value, hops):
        return lax.ppermute(value, ("y", "head"), [(a * 2 + c, b * 2 + d) for a, c, b, d in hops])

    outer = [(1, 2), (0, 3), (3, 0), (2, 1)]

    def first_hop(value):
        across = along(value, [(a, a // 2, a ^ 1, a // 2) for a in range(4)])
        return across, along(value, [(a, a // 2, b, a // 2) for a, b in outer])

    across_top, outward_top = first_hop(made_top)
    across_bottom, outward_bottom = first_hop(made_bottom)

    partial, top, bottom = kernel_call(
        apply_body,
        [shape(384, 1024, dtype=f32), shape(64, 1024), shape(64, 1024)],
        [place, query_half, out_own, moment_other, made_top, made_bottom],
        flops=2 * 512**3 * 5,
        scratch=[
            pltpu.VMEM((512, 512), bf16),
            pltpu.VMEM((2, 512, 512), f32),
            pltpu.VMEM((512, 512), bf16),
            pltpu.VMEM((512, 512), f32),
            pltpu.VMEM((512, 256), bf16),
            pltpu.VMEM((512, 256), bf16),
            pltpu.VMEM((4, 512, 256), f32),
        ],
    )
    low, high = kernel_call(
        relay_body,
        [shape(128, 1024)] * 2,
        [place, partial, moved(top, "y", 1), moved(bottom, "y", -1)],
    )
    relayed = along(across_top, [(a, a // 2, b, a // 2) for a, b in outer])
    traded = along(outward_bottom, [(a, 1 - a // 2, a ^ 1, 1 - a // 2) for a in range(4)])

    def emit(body, values, **more):
        count = len(values)
        return pl.pallas_call(
            body,
            out_shape=shape(2, 3, 512, 512),
            in_specs=[pl.BlockSpec(memory_space=pltpu.SMEM)]
            + [pl.BlockSpec(memory_space=pltpu.VMEM)] * count
            + [pl.BlockSpec(memory_space=pl.ANY)] * (len(more) > 0),
            out_specs=pl.BlockSpec(memory_space=pl.ANY),
            scratch_shapes=[pltpu.SemaphoreType.DMA((4,))],
            compiler_params=pltpu.CompilerParams(vmem_limit_bytes=16 << 20),
            cost_estimate=pl.CostEstimate(flops=0, bytes_accessed=3 << 20, transcendentals=0),
            **({"input_output_aliases": {count + 1: 0}} if more else {}),
        )(place, *values, *more.values())

    fast_next = emit(
        emit_body, (made_top, made_bottom, across_top, across_bottom, outward_top, outward_bottom)
    )
    fast_next = emit(finish_body, (relayed, traded), base=fast_next)
    sent_low, sent_high = moved(low, "y", -1), moved(high, "y", 1)
    layer_out = kernel_call(
        total_body, shape(128, 1024), [place, group_in[0], partial, sent_low, sent_high]
    )
    handed = moved(layer_out[None], "section", 1)
    return (handed, fast_next[None])


def solution(mesh):
    torus = Mesh(
        mesh.devices.reshape(mesh.shape["section"], 8, 4, mesh.shape["head"]),
        ("section", "z", "y", "head"),
    )
    return jax.shard_map(
        section_step,
        mesh=torus,
        in_specs=(
            P("section", TOK, None),
            P("section", None, TOK, "head"),
            P("section", "head", TOK),
            P("section", TOK, "head"),
            P("section", "head", None, None, None),
            P("section", "head", None, None, None),
            P("section", "head"),
            P("section", "head"),
        ),
        out_specs=(P("section", TOK, "head"), P("section", "head", None, None, None)),
        check_vma=False,
    )
```
